128 devices in a mesh: sa: 8 (over x, core), an: 16 (over y, z).
Axes of the slice: x: 4, y: 4, z: 4, core: 2. Of those that a mesh axis runs over, the one named last changes fastest.
Arguments:
- decoder_states: bfloat16 [8192, 4096], P('sa', 'an'), may hold values from -170 to 170
- w_query: bfloat16 [4096, 4096], P(None, 'an'), may hold values from -0.09375 to 0.09375
- w_key: bfloat16 [1024, 4096], P(None, 'an'), may hold values from -0.1875 to 0.1875
- w_value: bfloat16 [1024, 4096], P(None, 'an'), may hold values from -0.1875 to 0.1875
- w_out: bfloat16 [4096, 4096], P('an'), may hold values from -0.375 to 0.375
- enc_up: bfloat16 [1024, 4096], replicated, may hold values from -0.1875 to 0.1875
- enc_down: bfloat16 [4096, 1024], replicated, may hold values from -0.09375 to 0.09375
- neighbour_inputs: bfloat16 [1024, 128, 1024], P(('sa', 'an')), may hold values from -6 to 6
- requests: int32 [256], P('sa'), may hold values from 0 to 127, as said below
Outputs:
- cross_output: bfloat16 [8192, 4096], P('sa', 'an')
The draws below stay inside these ranges and needn't reach their ends.
Inputs may be any that keep to these rules, and one draw needn't show every extreme that they name: Within each block of 32 requests (one index of sa) the owner of a request is its value // 8; no owner receives more than 4 requests of a block and no more than 2 distinct neighbours of one owner are requested in a block; in every block some owner receives exactly 4 requests, 2 of them distinct. A neighbour may be requested several times.
All inputs are finite; a program needn't handle non-finite values.
Results may differ from the reference program's by a relative error of at most 0.01.
The reference program's roundings to bfloat16 on the way (of `chosen`, `normed`, `hidden`, `encoded`, `queries`, `probs` and `attended`) count: a program that leaves them out, or rounds other values in their place, can miss the bound.
Values may be sent and summed in bfloat16 or wider, within the bound.
A program may use at most 128 MiB of HBM per device.

```python
import jax
import jax.numpy as jnp
import numpy as np
from jax import lax

D = 4096
HEADS = 32
E = 1024
FFE = 4096
GROUP = 64
NT = 128
NEIGH = 2
CH_ROW = 16
NB_OWN = 8
TOKENS = 8192
POOL = 1024
N_SA = 8
N_AN = 16


def draw_decoder_states(key, part):
    first = jax.random.fold_in(key, 0)
    base = jax.random.normal(first, (TOKENS, D), jnp.float32)
    return jnp.clip(base, -6.0, 6.0).astype(jnp.bfloat16)


def draw_requests(key, part):
    average = NEIGH * CH_ROW // N_AN
    counts = np.array([2 * average if o % 4 == 0 else average if o % 4 == 1 else average // 2 for o in range(N_AN)])
    distinct = np.maximum(counts // 2, 1)
    slot_table = np.repeat(np.arange(N_AN), counts)
    within = np.concatenate([np.arange(c) for c in counts])
    repeat_of = within % distinct[slot_table]

    def one_row(row_key):
        key_list = jax.random.split(row_key, N_AN + 2)
        owners = jax.random.permutation(key_list[0], N_AN)
        local_ids = jax.vmap(lambda k: jax.random.permutation(k, NB_OWN))(key_list[2:])
        pool_ids = owners[slot_table] * NB_OWN + local_ids[slot_table, repeat_of]
        shuffle = jax.random.permutation(key_list[1], NEIGH * CH_ROW)
        return pool_ids[shuffle]
    all_rows = jax.vmap(one_row)(jax.random.split(jax.random.fold_in(key, 7), N_SA))
    return all_rows.reshape(-1).astype(jnp.int32)


def with_spikes(drawn, key, source, target, shards_of, factor):
    owner, partner = [(jnp.arange(drawn.shape[position]) // (drawn.shape[position] // shards_of)).reshape([-1 if axis == position else 1 for axis in range(drawn.ndim)]) for position in (source, target)]
    chosen = jax.random.permutation(key, shards_of)[partner]
    strong = (owner == chosen) | (owner == (partner + shards_of // 2) % shards_of)
    return jnp.where(strong, factor * drawn, drawn)


def block_scale(stream_key, shape, pieces, least, largest):
    loudness, own = 1.0, jax.random.fold_in(stream_key, 6)
    for dim, blocks in pieces:
        steps = jnp.exp(jax.random.uniform(jax.random.fold_in(own, dim), (blocks,), jnp.float32, least / len(pieces), largest / len(pieces)))
        loudness = loudness * jnp.repeat(steps, shape[dim] // blocks).reshape([-1 if axis == dim else 1 for axis in range(len(shape))])
    return loudness


def bell_draw(own_key, dims, scale, bound, pieces=(), held_as=jnp.bfloat16):
    level = block_scale(own_key, dims, pieces, -0.22, 0.18) if pieces else 1.0
    result = jax.random.normal(own_key, dims, jnp.float32) * scale * level
    return jnp.minimum(jnp.maximum(result, -bound), bound).astype(held_as)


def noise_with(key, dims, spread, reach, cuts, heavy, kind=jnp.bfloat16):
    values = spread * jax.random.normal(key, dims, jnp.float32)
    if cuts:
        values = values * block_scale(key, dims, cuts, -0.22, 0.18)
    return jnp.clip(with_spikes(values, jax.random.fold_in(key, 3), *heavy), -reach, reach).astype(kind)


def setup_inputs(seed: int = 0) -> dict:
    arg_keys = jax.random.split(jax.random.key(seed), 10)
    return {
        "decoder_states": draw_decoder_states(jax.random.fold_in(arg_keys[9], 71), 0),
        "w_query": bell_draw(arg_keys[1], (D, D), D ** -0.5, 0.09375, ((1, 16),)),
        "w_key": bell_draw(arg_keys[2], (E, D), E ** -0.5, 0.1875, ((1, 16),)),
        "w_value": bell_draw(arg_keys[3], (E, D), E ** -0.5, 0.1875, ((1, 16),)),
        "w_out": noise_with(arg_keys[4], (D, D), (D // 8) ** -0.5, 0.375, ((0, 16),), (0, 1, 16, 2.0)),
        "enc_up": bell_draw(arg_keys[5], (E, FFE), E ** -0.5, 0.1875),
        "enc_down": bell_draw(arg_keys[6], (FFE, E), FFE ** -0.5, 0.09375),
        "neighbour_inputs": bell_draw(arg_keys[7], (POOL, NT, E), 1.0, 6.0, ((0, 128),)),
        "requests": draw_requests(jax.random.fold_in(arg_keys[9], 71), 0),
    }


EPS = 1e-06

def encode(rows, enc_up, enc_down):
    wide = rows.astype(jnp.float32)
    square = lax.optimization_barrier(jnp.mean(wide * wide, axis=-1, keepdims=True))
    normed = (wide * lax.rsqrt(square + EPS)).astype(jnp.bfloat16)
    hidden = jax.nn.gelu(jnp.dot(normed, enc_up, preferred_element_type=jnp.float32), approximate=False).astype(jnp.bfloat16)
    return (wide + jnp.dot(hidden, enc_down, preferred_element_type=jnp.float32)).astype(jnp.bfloat16)

def reference(decoder_states, w_query, w_key, w_value, w_out, enc_up, enc_down, neighbour_inputs, requests):
    head_dim = D // HEADS
    scale = float(head_dim) ** (-0.5)
    tok_row = CH_ROW * GROUP
    req_row = NEIGH * CH_ROW
    pool_row = N_AN * NB_OWN

    def one_row(row):
        states = lax.dynamic_slice_in_dim(decoder_states, row * tok_row, tok_row, 0)
        wanted = lax.dynamic_slice_in_dim(requests, row * req_row, req_row, 0)
        pool = lax.dynamic_slice_in_dim(neighbour_inputs, row * pool_row, pool_row, 0)
        chosen = pool[wanted].reshape(req_row * NT, E)
        encoded = encode(chosen, enc_up, enc_down)
        keys = jnp.dot(encoded, w_key, preferred_element_type=jnp.float32).astype(jnp.bfloat16)
        values = jnp.dot(encoded, w_value, preferred_element_type=jnp.float32).astype(jnp.bfloat16)
        keys = keys.reshape(CH_ROW, NEIGH * NT, HEADS, head_dim).astype(jnp.float32)
        values = values.reshape(CH_ROW, NEIGH * NT, HEADS, head_dim).astype(jnp.float32)
        queries = jnp.dot(states, w_query, preferred_element_type=jnp.float32).astype(jnp.bfloat16)
        queries = queries.reshape(CH_ROW, GROUP, HEADS, head_dim).astype(jnp.float32)
        scores = jnp.einsum('cqhd,ckhd->chqk', queries, keys) * scale
        top = lax.optimization_barrier(jnp.max(scores, axis=-1, keepdims=True))
        weights = jnp.exp(scores - top)
        probs = (weights / lax.optimization_barrier(jnp.sum(weights, axis=-1, keepdims=True))).astype(jnp.bfloat16)
        attended = jnp.einsum('chqk,ckhd->cqhd', probs.astype(jnp.float32), values).astype(jnp.bfloat16)
        attended = attended.reshape(tok_row, D)
        return jnp.dot(attended, w_out, preferred_element_type=jnp.float32).astype(jnp.bfloat16)
    outputs = lax.map(one_row, jnp.arange(N_SA, dtype=jnp.int32))
    return outputs.reshape(N_SA * tok_row, D)
```

```python
import functools

import jax
import jax.numpy as jnp
from jax import lax
from jax.experimental import pallas as pl
from jax.experimental.pallas import tpu as pltpu
from jax.sharding import PartitionSpec as P

HEAD = 128
GROUP = 64
NEIGH = 2
EPS = 1e-06
SIDE = 4
PLANE = SIDE * SIDE
LINE = 8
FCHUNK = 512
MESSAGES = 20
F32 = jnp.float32
BF16 = jnp.bfloat16


class Gather:
    def __init__(self, number, buf, send, recv, row, y, z):
        self.number, self.buf, self.send, self.recv = number, buf, send, recv
        self.row, self.y, self.z = row, y, z
        self.half = buf.shape[1] // 2

    def block(self, h, dp, dq):
        dy = dp * (1 - h) + dq * h
        dz = dq * (1 - h) + dp * h
        return ((self.y + dy) % SIDE) * SIDE + (self.z + dz) % SIDE

    def copy(self, h, msg, dp, dq, part, to):
        rows = self.half
        first = h * rows
        if part is not None:
            rows = rows // 2
            first += part * rows
        ref = self.buf.at[self.block(h, dp, dq), pl.ds(first, rows)]
        k = h * MESSAGES + msg
        return pltpu.make_async_remote_copy(
            src_ref=ref,
            dst_ref=ref,
            send_sem=self.send.at[self.number, k],
            recv_sem=self.recv.at[self.number, k],
            device_id={"sa": self.row, "an": self.block(h, *to)},
            device_id_type=pl.DeviceIdType.MESH,
        )

    def first_ring(self, h):
        self.copy(h, 0, 0, 0, None, (1, 0)).start()
        self.copy(h, 1, 0, 0, None, (3, 0)).start()

    def second_ring(self, h, i):
        self.copy(h, 4 + i, i, 0, None, (0, 1)).start()
        self.copy(h, 8 + i, i, 0, None, (0, 3)).start()

    def wait(self, h, msg, dp, dq, part):
        self.copy(h, msg, dp, dq, part, (1, 0)).wait_recv()

    def event1(self):
        for h in (0, 1):
            self.wait(h, 0, 3, 0, None)
            self.copy(h, 2, 3, 0, 0, (1, 0)).start()
            self.second_ring(h, 3)
        for h in (0, 1):
            self.wait(h, 1, 1, 0, None)
            self.copy(h, 3, 1, 0, 1, (3, 0)).start()
            self.second_ring(h, 1)

    def pass_on(self, h, i):
        self.wait(h, 4 + i, i, 3, None)
        self.copy(h, 12 + i, i, 3, 0, (0, 1)).start()
        self.wait(h, 8 + i, i, 1, None)
        self.copy(h, 16 + i, i, 1, 1, (0, 3)).start()

    def event2(self):
        for h in (0, 1):
            self.pass_on(h, 0)

    def event3(self):
        for h in (0, 1):
            self.wait(h, 2, 2, 0, 0)
            self.wait(h, 3, 2, 0, 1)
            self.second_ring(h, 2)

    def event4(self):
        for i in (3, 1):
            for h in (0, 1):
                self.pass_on(h, i)

    def event5(self):
        for h in (0, 1):
            self.pass_on(h, 2)

    def event6(self):
        for i in (0, 3, 1, 2):
            for h in (0, 1):
                self.wait(h, 12 + i, i, 2, 0)
                self.wait(h, 16 + i, i, 2, 1)

    def sent(self):
        for h in (0, 1):
            for msg in range(MESSAGES):
                part = None if msg < 2 or 4 <= msg < 12 else 0
                self.copy(h, msg, 0, 0, part, (1, 0)).wait_send()


ARRIVED = {
    0: (2, lambda i: (i, 0, 0)),
    1: (4, lambda i: (i // 2, 1 + 2 * (i % 2), 0)),
    2: (4, lambda i: (i // 2, 0, 1 + 2 * (i % 2))),
    3: (2, lambda i: (i, 2, 0)),
    4: (8, lambda i: (i // 4, 1 + 2 * ((i // 2) % 2), 1 + 2 * (i % 2))),
    5: (4, lambda i: (i // 2, 2, 1 + 2 * (i % 2))),
    6: (8, lambda i: (i // 4, i % 4, 2)),
}


def body(
    table, states, w_query, w_key, w_value, w_out, enc_up, enc_down, nearby, out,
    sgat, egat, agat, wcol, wq, wkv, wrow, up, down, pool,
    wide, normed, qs, keys, vals, total,
    send, recv, wsend, wrecv, lsend, lrecv, local, wsem,
):
    row = lax.axis_index("sa")
    me = lax.axis_index("an")
    y, z = me // SIDE, me % SIDE
    tokens, width = states.shape
    wrows = w_out.shape[0] // LINE
    chunks = enc_up.shape[1] // FCHUNK

    loads = [
        pltpu.make_async_copy(states, sgat.at[me], local.at[0]),
        pltpu.make_async_copy(w_out.at[pl.ds(row * wrows, wrows)], wrow, local.at[1]),
        pltpu.make_async_copy(nearby, pool, local.at[2]),
        pltpu.make_async_copy(w_query, wq, local.at[3]),
        pltpu.make_async_copy(w_key, wkv.at[:, pl.ds(0, width)], local.at[4]),
        pltpu.make_async_copy(w_value, wkv.at[:, pl.ds(width, width)], local.at[5]),
        pltpu.make_async_copy(
            w_out.at[pl.ds(row * wrows, wrows), pl.ds(me * width, width)],
            wcol.at[me, row],
            local.at[6],
        ),
    ]

    def load_up(f):
        cut = pl.ds(f * FCHUNK, FCHUNK)
        return pltpu.make_async_copy(enc_up.at[:, cut], up.at[:, cut], wsem.at[0, f])

    def load_down(f):
        cut = pl.ds(f * FCHUNK, FCHUNK)
        return pltpu.make_async_copy(enc_down.at[cut], down.at[cut], wsem.at[1, f])

    for i in (0, 2, 1, 6):
        loads[i].start()
    for f in range(chunks):
        load_up(f).start()
        load_down(f).start()
    for i in (4, 5, 3):
        loads[i].start()

    barrier = pltpu.get_barrier_semaphore()

    def greet_plane(k, carry):
        pl.semaphore_signal(
            barrier, inc=1, device_id={"sa": row, "an": (me + k) % PLANE},
            device_id_type=pl.DeviceIdType.MESH,
        )
        return carry

    def greet_line(k, carry):
        pl.semaphore_signal(
            barrier, inc=1, device_id={"sa": (row + k) % LINE, "an": me},
            device_id_type=pl.DeviceIdType.MESH,
        )
        return carry

    lax.fori_loop(1, PLANE, greet_plane, 0)
    lax.fori_loop(1, LINE, greet_line, 0)
    pl.semaphore_wait(barrier, PLANE - 1 + LINE - 1)

    gs = Gather(0, sgat, send, recv, row, y, z)
    ge = Gather(1, egat, send, recv, row, y, z)
    ga = Gather(2, agat, send, recv, row, y, z)

    loads[0].wait()
    gs.first_ring(0)
    gs.first_ring(1)
    gs.second_ring(1, 0)
    gs.second_ring(0, 0)

    def plane_copy(k):
        to = (me + k) % PLANE
        return pltpu.make_async_remote_copy(
            src_ref=wrow.at[:, pl.ds(pl.multiple_of(to * width, width), width)],
            dst_ref=wcol.at[me, row],
            send_sem=wsend.at[k],
            recv_sem=wrecv.at[k],
            device_id={"sa": row, "an": to},
            device_id_type=pl.DeviceIdType.MESH,
        )

    def plane_arrival(k):
        return pltpu.make_async_remote_copy(
            src_ref=wcol.at[(me + PLANE - k) % PLANE, row],
            dst_ref=wcol.at[(me + PLANE - k) % PLANE, row],
            send_sem=wsend.at[k],
            recv_sem=wrecv.at[k],
            device_id={"sa": row, "an": (me + k) % PLANE},
            device_id_type=pl.DeviceIdType.MESH,
        )

    def line_copy(k, held):
        return pltpu.make_async_remote_copy(
            src_ref=wcol.at[:, held],
            dst_ref=wcol.at[:, held],
            send_sem=lsend.at[k],
            recv_sem=lrecv.at[k],
            device_id={"sa": (row + k) % LINE, "an": me},
            device_id_type=pl.DeviceIdType.MESH,
        )

    def repeat(first, last, step):
        def one(k, carry):
            step(k)
            return carry

        lax.fori_loop(first, last, one, 0)

    loads[1].wait()
    repeat(1, PLANE, lambda k: plane_copy(k).start())

    loads[2].wait()
    span = pool.shape[1]
    for slot in range(NEIGH):
        rows = pool[table[32 + slot]].astype(F32)
        cut = pl.ds(slot * span, span)
        wide[cut] = rows
        square = jnp.mean(rows * rows, axis=-1, keepdims=True)
        normed[cut] = (rows * lax.rsqrt(square + EPS)).astype(BF16)

    def encode_chunk(f):
        load_up(f).wait()
        load_down(f).wait()
        cut = pl.ds(pl.multiple_of(f * FCHUNK, FCHUNK), FCHUNK)
        pre = jnp.dot(normed[...], up[:, cut], preferred_element_type=F32)
        hidden = (0.5 * pre * (1.0 + lax.erf(pre * 0.5**0.5))).astype(BF16)
        wide[...] += jnp.dot(hidden, down[cut], preferred_element_type=F32)

    repeat(0, 3, encode_chunk)
    gs.event1()
    repeat(3, 6, encode_chunk)
    gs.event2()
    gs.event3()
    loads[6].wait()
    repeat(1, PLANE, lambda k: plane_arrival(k).wait_recv())
    repeat(1, LINE, lambda k: line_copy(k, row).start())
    repeat(6, chunks, encode_chunk)
    egat[me] = wide[...].astype(BF16)
    gs.event4()
    ge.first_ring(0)
    ge.first_ring(1)
    ge.second_ring(1, 0)
    ge.second_ring(0, 0)
    gs.event5()
    loads[4].wait()
    loads[5].wait()

    def project(i, where):
        h, dp, dq = where(i)
        slot = ge.block(h, dp, dq) * NEIGH + h
        cut = pl.ds(pl.multiple_of(h * span, span), span)
        both = jnp.dot(egat[ge.block(h, dp, dq), cut], wkv[...], preferred_element_type=F32)
        keys[slot] = both[:, :width].astype(BF16)
        vals[slot] = both[:, width:].astype(BF16)

    def on_arrival(event, work):
        count, where = ARRIVED[event]
        repeat(0, count, lambda i: work(i, where))

    gs.event6()
    ge.event1()
    loads[3].wait()

    def query_tile(t):
        cut = pl.ds(pl.multiple_of(t * 256, 256), 256)
        acc = jnp.zeros((256, width), F32)
        for j in range(PLANE):
            acc = acc + jnp.dot(
                sgat[j, cut], wq[j * width : (j + 1) * width], preferred_element_type=F32
            )
        qs[cut] = acc.astype(BF16)

    on_arrival(0, project)
    on_arrival(1, project)
    ge.event2()
    on_arrival(2, project)
    ge.event3()
    on_arrival(3, project)
    repeat(0, tokens // 256, query_tile)
    ge.event4()
    on_arrival(4, project)
    ge.event5()
    on_arrival(5, project)
    ge.event6()
    on_arrival(6, project)

    scale = float(HEAD) ** -0.5

    def attend(g):
        cut = pl.ds(pl.multiple_of(g * GROUP, GROUP), GROUP)
        one, two = table[NEIGH * g], table[NEIGH * g + 1]
        k = jnp.concatenate([keys[one], keys[two]], axis=0)
        v = jnp.concatenate([vals[one], vals[two]], axis=0)
        q = qs[cut]
        done = []
        for h in range(width // HEAD):
            part = slice(h * HEAD, (h + 1) * HEAD)
            scores = lax.dot_general(
                q[:, part], k[:, part], (((1,), (1,)), ((), ())), preferred_element_type=F32
            ) * scale
            weights = jnp.exp(scores - jnp.max(scores, axis=-1, keepdims=True))
            probs = weights / jnp.sum(weights, axis=-1, keepdims=True)
            done.append(jnp.dot(probs.astype(BF16), v[:, part], preferred_element_type=F32))
        agat[me, cut] = jnp.concatenate(done, axis=1).astype(BF16)

    groups = tokens // GROUP
    lax.fori_loop(0, groups // 4, lambda g, c: (attend(2 * g), attend(2 * g + 1), c)[2], 0)
    ga.first_ring(0)
    ga.second_ring(0, 0)
    lax.fori_loop(groups // 4, groups // 2, lambda g, c: (attend(2 * g), attend(2 * g + 1), c)[2], 0)
    ga.first_ring(1)
    ga.second_ring(1, 0)

    repeat(1, LINE, lambda k: line_copy(k, (row + LINE - k) % LINE).wait_recv())
    total[...] = jnp.zeros_like(total)

    def add_output(i, where):
        h, dp, dq = where(i)
        j = ga.block(h, dp, dq)
        half = tokens // 2
        cut = pl.ds(pl.multiple_of(h * half, half), half)
        total[cut] += jnp.dot(
            agat[j, cut], wcol[j].reshape(width, width), preferred_element_type=F32
        )

    on_arrival(0, add_output)
    ga.event1()
    on_arrival(1, add_output)
    ga.event2()
    on_arrival(2, add_output)
    ga.event3()
    on_arrival(3, add_output)
    ga.event4()
    on_arrival(4, add_output)
    ga.event5()
    on_arrival(5, add_output)
    ga.event6()
    on_arrival(6, add_output)
    out[...] = total[...].astype(BF16)

    for gather in (gs, ge, ga):
        gather.sent()
    repeat(1, PLANE, lambda k: plane_copy(k).wait_send())
    repeat(1, LINE, lambda k: line_copy(k, row).wait_send())


def request_table(requests, own, position):
    owner = requests // own
    same = owner[:, None] == owner[None, :]
    rank = jnp.any(same & (requests[None, :] < requests[:, None]), axis=1)
    slot = owner * NEIGH + rank.astype(jnp.int32)
    mine = owner == position
    low = jnp.min(jnp.where(mine, requests % own, own - 1))
    high = jnp.max(jnp.where(mine, requests % own, 0))
    return jnp.concatenate([slot, jnp.stack([low, high])]).astype(jnp.int32)


def shards(
    decoder_states, w_query, w_key, w_value, w_out, enc_up, enc_down, neighbour_inputs, requests
):
    tokens, width = decoder_states.shape
    own, span, features = neighbour_inputs.shape
    table = request_table(requests, own, lax.axis_index("an"))
    hbm = pl.BlockSpec(memory_space=pl.ANY)
    slots = PLANE * NEIGH
    chunks = enc_up.shape[1] // FCHUNK
    return pl.pallas_call(
        body,
        out_shape=jax.ShapeDtypeStruct((tokens, width), BF16),
        in_specs=[pl.BlockSpec(memory_space=pltpu.SMEM)] + [hbm] * 8,
        out_specs=pl.BlockSpec(memory_space=pltpu.VMEM),
        scratch_shapes=[
            pltpu.VMEM((PLANE, tokens, width), BF16),
            pltpu.VMEM((PLANE, NEIGH * span, features), BF16),
            pltpu.VMEM((PLANE, tokens, width), BF16),
            pltpu.VMEM((PLANE, LINE, w_out.shape[0] // LINE, width), BF16),
            pltpu.VMEM(w_query.shape, BF16),
            pltpu.VMEM((features, 2 * width), BF16),
            pltpu.VMEM((w_out.shape[0] // LINE, w_out.shape[1]), BF16),
            pltpu.VMEM(enc_up.shape, BF16),
            pltpu.VMEM(enc_down.shape, BF16),
            pltpu.VMEM(neighbour_inputs.shape, BF16),
            pltpu.VMEM((NEIGH * span, features), F32),
            pltpu.VMEM((NEIGH * span, features), BF16),
            pltpu.VMEM((tokens, width), BF16),
            pltpu.VMEM((slots, span, width), BF16),
            pltpu.VMEM((slots, span, width), BF16),
            pltpu.VMEM((tokens, width), F32),
            pltpu.SemaphoreType.DMA((3, 2 * MESSAGES)),
            pltpu.SemaphoreType.DMA((3, 2 * MESSAGES)),
            pltpu.SemaphoreType.DMA((PLANE,)),
            pltpu.SemaphoreType.DMA((PLANE,)),
            pltpu.SemaphoreType.DMA((LINE,)),
            pltpu.SemaphoreType.DMA((LINE,)),
            pltpu.SemaphoreType.DMA((7,)),
            pltpu.SemaphoreType.DMA((2, chunks)),
        ],
        compiler_params=pltpu.CompilerParams(
            collective_id=0, has_side_effects=True, vmem_limit_bytes=67043328
        ),
    )(
        table, decoder_states, w_query, w_key, w_value, w_out, enc_up, enc_down, neighbour_inputs
    )


def solution(mesh):
    placed = (
        P("sa", "an"),
        P(None, "an"),
        P(None, "an"),
        P(None, "an"),
        P("an", None),
        P(),
        P(),
        P(("sa", "an"), None, None),
        P("sa"),
    )
    return jax.shard_map(
        shards, mesh=mesh, in_specs=placed, out_specs=P("sa", "an"), check_vma=False
    )
```

```python
import functools

import jax
import jax.numpy as jnp
from jax import lax
from jax.experimental import pallas as pl
from jax.experimental.pallas import tpu as pltpu
from jax.sharding import PartitionSpec as P

HEAD = 128
GROUP = 64
NEIGH = 2
EPS = 1e-06
SIDE = 4
PLANE = SIDE * SIDE
LINE = 8
FCHUNK = 512
CORES = 2
PAIR = 2
F32 = jnp.float32
BF16 = jnp.bfloat16


class Gather:
    def __init__(self, number, buf, send, recv, place):
        self.number, self.buf, self.send, self.recv = number, buf, send, recv
        self.place = place
        self.half = buf.shape[1] // 2

    def copy(self, lane, h, k, dy, db, part, to):
        rows = self.half
        first = h * rows
        if part is not None:
            rows = rows // 2
            first += part * rows
        ref = self.buf.at[self.place.block(lane, dy, db), pl.ds(first, rows)]
        return pltpu.make_async_remote_copy(
            src_ref=ref,
            dst_ref=ref,
            send_sem=self.send.at[self.number, k],
            recv_sem=self.recv.at[self.number, k],
            device_id=to,
            device_id_type=pl.DeviceIdType.MESH,
        )

    def message(self, name, i=0):
        p = self.place
        up, dn, pair = p.ring(1), p.ring(3), p.pair
        if name == "a_up":
            return 0, 0, (0, 0), (3, 0), None, up
        if name == "a_dn":
            return 0, 1, (0, 0), (1, 0), None, dn
        if name == "a_up2":
            return 0, 2, (3, 0), (2, 0), 0, up
        if name == "a_dn2":
            return 0, 3, (1, 0), (2, 0), 1, dn
        if name == "a_pair":
            return 0, 4 + i, (i, 0), (i, 1), None, pair
        if name == "b_pair":
            return 1, 8, (0, 0), (0, 1), None, pair
        if name == "b_up":
            return 1, 9 + i, (0, i), (3, i), None, up
        if name == "b_dn":
            return 1, 11 + i, (0, i), (1, i), None, dn
        if name == "b_up2":
            return 1, 13 + i, (3, i), (2, i), 0, up
        assert name == "b_dn2"
        return 1, 15 + i, (1, i), (2, i), 1, dn

    def go(self, name, i=0):
        h, k, sent, _, part, to = self.message(name, i)
        self.copy(0, h, k, *sent, part, to).start()

    def get(self, name, i=0):
        h, k, _, got, part, to = self.message(name, i)
        self.copy(0, h, k, *got, part, to).wait_recv()

    def across(self, lane, unit):
        h, dy, db = unit
        k = ROUTED + h * 8 + dy * PAIR + db
        return self.copy(lane, h, k, dy, db, None, self.place.twin)

    def share(self, units):
        for unit in units:
            self.across(0, unit).start()

    def shared(self, event):
        for unit in UNITS[event]:
            self.across(1, unit).wait_recv()

    def own(self, h):
        if h == 0:
            self.go("a_up")
            self.go("a_dn")
            self.go("a_pair", 0)
        else:
            self.go("b_pair")
            self.go("b_up", 0)
            self.go("b_dn", 0)
        self.share([UNITS[0][h]])

    def event(self, e):
        if e == 1:
            self.get("a_up")
            self.go("a_up2")
            self.go("a_pair", 3)
            self.get("a_dn")
            self.go("a_dn2")
            self.go("a_pair", 1)
            self.get("b_pair")
            self.go("b_up", 1)
            self.go("b_dn", 1)
        elif e == 2:
            self.get("b_up", 0)
            self.go("b_up2", 0)
            self.get("b_dn", 0)
            self.go("b_dn2", 0)
            self.get("a_pair", 0)
        elif e == 3:
            self.get("a_up2")
            self.get("a_dn2")
            self.go("a_pair", 2)
        elif e == 4:
            self.get("b_up", 1)
            self.go("b_up2", 1)
            self.get("b_dn", 1)
            self.go("b_dn2", 1)
        elif e == 5:
            self.get("a_pair", 3)
            self.get("a_pair", 1)
        else:
            for i in (0, 1):
                self.get("b_up2", i)
                self.get("b_dn2", i)
            self.get("a_pair", 2)
        self.share(UNITS[e])

    def sent(self):
        for name, count in MESSAGES:
            for i in range(count):
                h, k, sent, _, part, to = self.message(name, i)
                self.copy(0, h, k, *sent, part, to).wait_send()
        for event in UNITS:
            for unit in UNITS[event]:
                self.across(0, unit).wait_send()


MESSAGES = (
    ("a_up", 1), ("a_dn", 1), ("a_up2", 1), ("a_dn2", 1), ("a_pair", 4),
    ("b_pair", 1), ("b_up", 2), ("b_dn", 2), ("b_up2", 2), ("b_dn2", 2),
)
ROUTED = 17
SWAP = 33
UNITS = {
    0: [(0, 0, 0), (1, 0, 0)],
    1: [(0, 3, 0), (0, 1, 0), (1, 0, 1)],
    2: [(1, 3, 0), (1, 1, 0), (0, 0, 1)],
    3: [(0, 2, 0)],
    4: [(1, 3, 1), (1, 1, 1)],
    5: [(0, 3, 1), (0, 1, 1)],
    6: [(1, 2, 0), (1, 2, 1), (0, 2, 1)],
}


class Place:
    def __init__(self):
        self.row = lax.axis_index("sa")
        self.me = lax.axis_index("an")
        self.x, self.c = self.row // CORES, self.row % CORES
        self.y, self.z = self.me // SIDE, self.me % SIDE
        self.s, self.b = self.z // PAIR, self.z % PAIR
        self.foreign = (self.c + self.s) % 2
        self.outer = self.y * SIDE + self.outer_z(self.z)
        self.mine = self.block(0, 0, 0)
        self.pair = {"sa": self.row, "an": self.y * SIDE + self.s * PAIR + 1 - self.b}
        self.twin = {"sa": self.row + 1 - 2 * self.c, "an": self.me}
        self.partner = {"sa": self.row + 1 - 2 * self.c, "an": self.outer}
        self.holder = {"sa": self.row, "an": self.outer}

    def outer_z(self, z):
        return (z + 2 * (z % PAIR) + 3) % SIDE

    def ring(self, dy):
        return {"sa": self.row, "an": ((self.y + dy) % SIDE) * SIDE + self.z}

    def block(self, lane, dy, db):
        foreign = (self.foreign + lane) % 2
        b = (self.b + db) % PAIR
        z = self.s * PAIR + b
        return ((self.y + dy) % SIDE) * SIDE + (z + foreign * (2 * b + 3)) % SIDE

    def task_of(self, an):
        y, z = an // SIDE, an % SIDE
        foreign = (self.c + z // PAIR) % 2
        return y * SIDE + (z + foreign * (2 * (z % PAIR) + 3)) % SIDE


def repeat(first, last, step):
    def one(k, carry):
        step(k)
        return carry

    lax.fori_loop(first, last, one, 0)


def either(flag, yes, no):
    pl.when(flag == 1)(yes)
    pl.when(flag == 0)(no)


def visit(own, shared, work):
    units = [(0,) + unit for unit in own] + [(1,) + unit for unit in shared]

    def one(i):
        picked = []
        for column in zip(*units):
            value = jnp.int32(column[0])
            for k in range(1, len(column)):
                value = jnp.where(i == k, jnp.int32(column[k]), value)
            picked.append(value)
        work(*picked)

    repeat(0, len(units), one)


def body(
    table, states, w_query, w_key, w_value, w_out, enc_up, enc_down, nearby, out,
    sgat, egat, agat, wcol, wq, wkv, wrow, up, down, pool,
    wide, normed, qs, keys, vals, total, arrived, other_table, local_table, task_table,
    send, recv, wsend, wrecv, lsend, lrecv, qsend, qrecv, local, wsem,
):
    p = Place()
    row, me, x, b = p.row, p.me, p.x, p.b
    tokens, width = states.shape
    wrows = w_out.shape[0] // LINE
    chunks = enc_up.shape[1] // FCHUNK
    share = x * PAIR + b

    def remote(src, dst, ssem, rsem, to):
        return pltpu.make_async_remote_copy(
            src_ref=src, dst_ref=dst, send_sem=ssem, recv_sem=rsem,
            device_id=to, device_id_type=pl.DeviceIdType.MESH,
        )

    load_states = pltpu.make_async_copy(states, sgat.at[me], local.at[0])
    load_rows = pltpu.make_async_copy(
        w_out.at[pl.ds(x * PAIR * wrows, PAIR * wrows)], wrow, local.at[1]
    )
    load_pool = pltpu.make_async_copy(nearby, pool, local.at[2])
    load_query = pltpu.make_async_copy(w_query, wq, local.at[3])
    load_key = pltpu.make_async_copy(w_key, wkv.at[:, pl.ds(0, width)], local.at[4])
    load_value = pltpu.make_async_copy(w_value, wkv.at[:, pl.ds(width, width)], local.at[5])
    load_column = pltpu.make_async_copy(
        w_out.at[
            pl.ds(pl.multiple_of(share * wrows, wrows), wrows),
            pl.ds(pl.multiple_of(p.mine * width, width), width),
        ],
        wcol.at[me, share],
        local.at[6],
    )
    load_table = pltpu.make_async_copy(table, local_table, local.at[7])

    def load_up(f):
        cut = pl.ds(pl.multiple_of(f * FCHUNK, FCHUNK), FCHUNK)
        return pltpu.make_async_copy(enc_up.at[:, cut], up.at[:, cut], wsem.at[0, f])

    def load_down(f):
        cut = pl.ds(pl.multiple_of(f * FCHUNK, FCHUNK), FCHUNK)
        return pltpu.make_async_copy(enc_down.at[cut], down.at[cut], wsem.at[1, f])

    def load_weights():
        load_key.start()
        load_value.start()
        load_query.start()

    pl.when(p.foreign == 0)(load_states.start)
    load_table.start()
    load_pool.start()
    load_rows.start()
    load_column.start()
    repeat(0, chunks, lambda f: (load_up(f).start(), load_down(f).start()))
    pl.when(p.foreign == 0)(load_weights)

    barrier = pltpu.get_barrier_semaphore()

    def greet(to):
        pl.semaphore_signal(barrier, inc=1, device_id=to, device_id_type=pl.DeviceIdType.MESH)

    def line(k):
        far = k % PAIR
        at = far * p.outer + (1 - far) * me
        return {"sa": ((x + k // PAIR) % SIDE) * CORES + p.c, "an": at}

    greet(p.partner)
    greet(p.twin)
    repeat(1, PLANE, lambda k: greet({"sa": row, "an": (me + k) % PLANE}))
    repeat(1, LINE, lambda k: greet(line(k)))
    pl.semaphore_wait(barrier, PLANE - 1 + LINE - 1 + 2)

    gs = Gather(0, sgat, send, recv, p)
    ge = Gather(1, egat, send, recv, p)
    ga = Gather(2, agat, send, recv, p)

    def swap(number, src, buf, to_slot):
        return remote(
            src, buf.at[to_slot], send.at[number, SWAP], recv.at[number, SWAP], p.partner
        )

    def swap_states():
        swap(0, states, sgat, me).start()
        swap(0, states, sgat, p.outer).wait_recv()

    either(p.foreign, swap_states, load_states.wait)
    gs.own(1)
    gs.own(0)

    table_copy = remote(table, other_table, qsend.at[0], qrecv.at[0], p.twin)
    table_copy.start()

    def plane_copy(k):
        an = (me + k) % PLANE
        part = an % PAIR
        task = p.task_of(an)
        return remote(
            wrow.at[
                pl.ds(pl.multiple_of(part * wrows, wrows), wrows),
                pl.ds(pl.multiple_of(task * width, width), width),
            ],
            wcol.at[me, x * PAIR + part],
            wsend.at[k],
            wrecv.at[k],
            {"sa": row, "an": an},
        )

    def plane_arrival(k):
        ref = wcol.at[(me + PLANE - k) % PLANE, share]
        return remote(ref, ref, wsend.at[k], wrecv.at[k], {"sa": row, "an": (me + k) % PLANE})

    def line_copy(k, held):
        ref = wcol.at[:, held]
        return remote(ref, ref, lsend.at[k], lrecv.at[k], line(k))

    def line_arrival(k):
        far = k % PAIR
        part = b + far * (1 - 2 * b)
        return line_copy(k, ((x + SIDE - k // PAIR) % SIDE) * PAIR + part)

    load_rows.wait()
    repeat(1, PLANE, lambda k: plane_copy(k).start())

    load_table.wait()
    load_pool.wait()
    span = pool.shape[1]
    for slot in range(NEIGH):
        rows = pool[local_table[0, 32 + slot]].astype(F32)
        cut = pl.ds(slot * span, span)
        wide[cut] = rows
        square = jnp.mean(rows * rows, axis=-1, keepdims=True)
        normed[cut] = (rows * lax.rsqrt(square + EPS)).astype(BF16)

    def encode_chunk(f):
        load_up(f).wait()
        load_down(f).wait()
        cut = pl.ds(pl.multiple_of(f * FCHUNK, FCHUNK), FCHUNK)
        pre = jnp.dot(normed[...], up[:, cut], preferred_element_type=F32)
        hidden = (0.5 * pre * (1.0 + lax.erf(pre * 0.5**0.5))).astype(BF16)
        wide[...] += jnp.dot(hidden, down[cut], preferred_element_type=F32)

    weight_copies = (
        remote(wkv, wkv, qsend.at[1], qrecv.at[1], p.holder),
        remote(wq, wq, qsend.at[2], qrecv.at[2], p.holder),
    )

    def give_weights():
        load_key.wait()
        load_value.wait()
        load_query.wait()
        for copy in weight_copies:
            copy.start()

    repeat(0, 2, encode_chunk)
    gs.event(1)
    pl.when(p.foreign == 0)(give_weights)
    repeat(2, 4, encode_chunk)
    gs.event(2)
    gs.event(3)
    repeat(4, 6, encode_chunk)
    gs.event(4)
    repeat(6, chunks, encode_chunk)

    def swap_encoded():
        normed[...] = wide[...].astype(BF16)
        swap(1, normed, egat, me).start()

    def keep_encoded():
        egat[me] = wide[...].astype(BF16)

    either(p.foreign, swap_encoded, keep_encoded)
    gs.event(5)
    pl.when(p.foreign == 1)(swap(1, normed, egat, p.outer).wait_recv)
    ge.own(1)
    ge.own(0)
    load_column.wait()
    repeat(1, PLANE, lambda k: plane_arrival(k).wait_recv())
    repeat(1, LINE, lambda k: line_copy(k, share).start())
    gs.event(6)

    def task_table_from(src):
        def copy():
            moved = pltpu.make_async_copy(src, task_table, local.at[8])
            moved.start()
            moved.wait()

        return copy

    table_copy.wait_recv()
    either(p.foreign, task_table_from(other_table), task_table_from(table))
    pl.when(p.foreign == 1)(weight_copies[0].wait_recv)

    def project(lane, h, dy, db):
        block = p.block(lane, dy, db)
        slot = block * NEIGH + h
        cut = pl.ds(pl.multiple_of(h * span, span), span)
        both = jnp.dot(egat[block, cut], wkv[...], preferred_element_type=F32)
        keys[slot] = both[:, :width].astype(BF16)
        vals[slot] = both[:, width:].astype(BF16)

    def query_tile(t):
        cut = pl.ds(pl.multiple_of(t * 256, 256), 256)
        acc = jnp.zeros((256, width), F32)
        for j in range(PLANE):
            acc = acc + jnp.dot(
                sgat[j, cut], wq[j * width : (j + 1) * width], preferred_element_type=F32
            )
        qs[cut] = acc.astype(BF16)

    ge.event(1)
    ge.shared(0)
    visit(UNITS[0] + UNITS[1], UNITS[0], project)
    ge.event(2)
    ge.shared(1)
    visit(UNITS[2], UNITS[1], project)
    ge.event(3)
    ge.shared(2)
    visit(UNITS[3], UNITS[2], project)
    for event in UNITS:
        gs.shared(event)
    pl.when(p.foreign == 1)(weight_copies[1].wait_recv)
    ge.event(4)
    repeat(0, tokens // 256, query_tile)
    ge.shared(3)
    visit(UNITS[4], UNITS[3], project)
    ge.event(5)
    ge.shared(4)
    visit(UNITS[5], UNITS[4], project)
    ge.event(6)
    ge.shared(5)
    visit(UNITS[6], UNITS[5], project)
    ge.shared(6)
    visit([], UNITS[6], project)

    scale = float(HEAD) ** -0.5

    def attend(g):
        cut = pl.ds(pl.multiple_of(g * GROUP, GROUP), GROUP)
        one, two = task_table[0, NEIGH * g], task_table[0, NEIGH * g + 1]
        k = jnp.concatenate([keys[one], keys[two]], axis=0)
        v = jnp.concatenate([vals[one], vals[two]], axis=0)
        q = qs[cut]
        done = []
        for h in range(width // HEAD):
            part = slice(h * HEAD, (h + 1) * HEAD)
            scores = lax.dot_general(
                q[:, part], k[:, part], (((1,), (1,)), ((), ())), preferred_element_type=F32
            ) * scale
            weights = jnp.exp(scores - jnp.max(scores, axis=-1, keepdims=True))
            probs = weights / jnp.sum(weights, axis=-1, keepdims=True)
            done.append(jnp.dot(probs.astype(BF16), v[:, part], preferred_element_type=F32))
        agat[p.mine, cut] = jnp.concatenate(done, axis=1).astype(BF16)

    pairs = tokens // GROUP // 2
    repeat(0, pairs // 2, lambda g: (attend(2 * g), attend(2 * g + 1)))
    ga.own(0)
    repeat(pairs // 2, pairs, lambda g: (attend(2 * g), attend(2 * g + 1)))
    ga.own(1)

    repeat(1, LINE, lambda k: line_arrival(k).wait_recv())
    total[...] = jnp.zeros_like(total)

    def add_output(lane, h, dy, db):
        j = p.block(lane, dy, db)
        half = tokens // 2
        cut = pl.ds(pl.multiple_of(h * half, half), half)
        total[cut] += jnp.dot(
            agat[j, cut], wcol[j].reshape(width, width), preferred_element_type=F32
        )

    visit(UNITS[0], [], add_output)
    for event in range(1, 7):
        ga.event(event)
        ga.shared(event - 1)
        visit(UNITS[event], UNITS[event - 1], add_output)
    ga.shared(6)
    visit([], UNITS[6], add_output)

    swap_out = remote(qs, arrived, send.at[2, SWAP], recv.at[2, SWAP], p.partner)

    def swap_output():
        qs[...] = total[...].astype(BF16)
        swap_out.start()
        swap_out.wait_recv()
        out[...] = arrived[...]

    def keep_output():
        out[...] = total[...].astype(BF16)

    either(p.foreign, swap_output, keep_output)

    for gather in (gs, ge, ga):
        gather.sent()
    table_copy.wait_send()

    def sent_foreign():
        swap(0, states, sgat, me).wait_send()
        swap(1, normed, egat, me).wait_send()
        swap_out.wait_send()

    def sent_home():
        for copy in weight_copies:
            copy.wait_send()

    either(p.foreign, sent_foreign, sent_home)
    repeat(1, PLANE, lambda k: plane_copy(k).wait_send())
    repeat(1, LINE, lambda k: line_copy(k, share).wait_send())


def request_table(requests, own, position):
    owner = requests // own
    same = owner[:, None] == owner[None, :]
    rank = jnp.any(same & (requests[None, :] < requests[:, None]), axis=1)
    slot = owner * NEIGH + rank.astype(jnp.int32)
    mine = owner == position
    low = jnp.min(jnp.where(mine, requests % own, own - 1))
    high = jnp.max(jnp.where(mine, requests % own, 0))
    packed = jnp.concatenate([slot, jnp.stack([low, high])]).astype(jnp.int32)
    return jnp.pad(packed, (0, HEAD - packed.shape[0]))[None, :]


def shards(
    decoder_states, w_query, w_key, w_value, w_out, enc_up, enc_down, neighbour_inputs, requests
):
    tokens, width = decoder_states.shape
    own, span, features = neighbour_inputs.shape
    table = request_table(requests, own, lax.axis_index("an"))
    hbm = pl.BlockSpec(memory_space=pl.ANY)
    slots = PLANE * NEIGH
    chunks = enc_up.shape[1] // FCHUNK
    return pl.pallas_call(
        body,
        out_shape=jax.ShapeDtypeStruct((tokens, width), BF16),
        in_specs=[pl.BlockSpec(memory_space=pltpu.VMEM)] + [hbm] * 8,
        out_specs=pl.BlockSpec(memory_space=pltpu.VMEM),
        scratch_shapes=[
            pltpu.VMEM((PLANE, tokens, width), BF16),
            pltpu.VMEM((PLANE, NEIGH * span, features), BF16),
            pltpu.VMEM((PLANE, tokens, width), BF16),
            pltpu.VMEM((PLANE, LINE, w_out.shape[0] // LINE, width), BF16),
            pltpu.VMEM(w_query.shape, BF16),
            pltpu.VMEM((features, 2 * width), BF16),
            pltpu.VMEM((PAIR * w_out.shape[0] // LINE, w_out.shape[1]), BF16),
            pltpu.VMEM(enc_up.shape, BF16),
            pltpu.VMEM(enc_down.shape, BF16),
            pltpu.VMEM(neighbour_inputs.shape, BF16),
            pltpu.VMEM((NEIGH * span, features), F32),
            pltpu.VMEM((NEIGH * span, features), BF16),
            pltpu.VMEM((tokens, width), BF16),
            pltpu.VMEM((slots, span, width), BF16),
            pltpu.VMEM((slots, span, width), BF16),
            pltpu.VMEM((tokens, width), F32),
            pltpu.VMEM((tokens, width), BF16),
            pltpu.VMEM((1, HEAD), jnp.int32),
            pltpu.SMEM((1, HEAD), jnp.int32),
            pltpu.SMEM((1, HEAD), jnp.int32),
            pltpu.SemaphoreType.DMA((3, SWAP + 1)),
            pltpu.SemaphoreType.DMA((3, SWAP + 1)),
            pltpu.SemaphoreType.DMA((PLANE,)),
            pltpu.SemaphoreType.DMA((PLANE,)),
            pltpu.SemaphoreType.DMA((LINE,)),
            pltpu.SemaphoreType.DMA((LINE,)),
            pltpu.SemaphoreType.DMA((3,)),
            pltpu.SemaphoreType.DMA((3,)),
            pltpu.SemaphoreType.DMA((9,)),
            pltpu.SemaphoreType.DMA((2, chunks)),
        ],
        compiler_params=pltpu.CompilerParams(
            collective_id=0, has_side_effects=True, vmem_limit_bytes=67043328
        ),
    )(
        table, decoder_states, w_query, w_key, w_value, w_out, enc_up, enc_down, neighbour_inputs
    )


def solution(mesh):
    placed = (
        P("sa", "an"),
        P(None, "an"),
        P(None, "an"),
        P(None, "an"),
        P("an", None),
        P(),
        P(),
        P(("sa", "an"), None, None),
        P("sa"),
    )
    return jax.shard_map(
        shards, mesh=mesh, in_specs=placed, out_specs=P("sa", "an"), check_vma=False
    )
```

```python
import functools

import jax
import jax.numpy as jnp
from jax import lax
from jax.experimental import pallas as pl
from jax.experimental.pallas import tpu as pltpu
from jax.sharding import PartitionSpec as P

HEAD = 128
GROUP = 64
NEIGH = 2
EPS = 1e-06
SIDE = 4
PLANE = SIDE * SIDE
LINE = 8
FCHUNK = 512
CORES = 2
PAIR = 2
LOG2E = 1.4426950408889634
F32 = jnp.float32
BF16 = jnp.bfloat16


class Gather:
    def __init__(self, number, buf, send, recv, place):
        self.number, self.buf, self.send, self.recv = number, buf, send, recv
        self.place = place
        self.half = buf.shape[1] // 2

    def copy(self, lane, h, k, dy, db, part, to):
        rows = self.half
        first = h * rows
        if part is not None:
            rows = rows // 2
            first += part * rows
        ref = self.buf.at[self.place.block(lane, dy, db), pl.ds(first, rows)]
        return pltpu.make_async_remote_copy(
            src_ref=ref,
            dst_ref=ref,
            send_sem=self.send.at[self.number, k],
            recv_sem=self.recv.at[self.number, k],
            device_id=to,
            device_id_type=pl.DeviceIdType.MESH,
        )

    def message(self, name, i=0):
        p = self.place
        up, dn, pair = p.ring(1), p.ring(3), p.pair
        if name == "a_up":
            return 0, 0, (0, 0), (3, 0), None, up
        if name == "a_dn":
            return 0, 1, (0, 0), (1, 0), None, dn
        if name == "a_up2":
            return 0, 2, (3, 0), (2, 0), 0, up
        if name == "a_dn2":
            return 0, 3, (1, 0), (2, 0), 1, dn
        if name == "a_pair":
            return 0, 4 + i, (i, 0), (i, 1), None, pair
        if name == "b_pair":
            return 1, 8, (0, 0), (0, 1), None, pair
        if name == "b_up":
            return 1, 9 + i, (0, i), (3, i), None, up
        if name == "b_dn":
            return 1, 11 + i, (0, i), (1, i), None, dn
        if name == "b_up2":
            return 1, 13 + i, (3, i), (2, i), 0, up
        assert name == "b_dn2"
        return 1, 15 + i, (1, i), (2, i), 1, dn

    def go(self, name, i=0):
        h, k, sent, _, part, to = self.message(name, i)
        self.copy(0, h, k, *sent, part, to).start()

    def get(self, name, i=0):
        h, k, _, got, part, to = self.message(name, i)
        self.copy(0, h, k, *got, part, to).wait_recv()

    def across(self, lane, unit):
        h, dy, db = unit
        k = ROUTED + h * 8 + dy * PAIR + db
        return self.copy(lane, h, k, dy, db, None, self.place.twin)

    def share(self, units):
        for unit in units:
            self.across(0, unit).start()

    def shared(self, event):
        for unit in UNITS[event]:
            self.across(1, unit).wait_recv()

    def own(self, h):
        if h == 0:
            self.go("a_up")
            self.go("a_dn")
            self.go("a_pair", 0)
        else:
            self.go("b_pair")
            self.go("b_up", 0)
            self.go("b_dn", 0)
        self.share([UNITS[0][h]])

    def own_both(self):
        self.go("b_pair")
        self.go("a_up")
        self.go("a_dn")
        self.go("a_pair", 0)
        self.go("b_up", 0)
        self.go("b_dn", 0)
        self.share(UNITS[0])

    def event(self, e):
        if e == 1:
            self.get("a_up")
            self.go("a_up2")
            self.go("a_pair", 3)
            self.get("a_dn")
            self.go("a_dn2")
            self.go("a_pair", 1)
            self.get("b_pair")
            self.go("b_up", 1)
            self.go("b_dn", 1)
        elif e == 2:
            self.get("b_up", 0)
            self.go("b_up2", 0)
            self.get("b_dn", 0)
            self.go("b_dn2", 0)
            self.get("a_pair", 0)
        elif e == 3:
            self.get("a_up2")
            self.get("a_dn2")
            self.go("a_pair", 2)
        elif e == 4:
            self.get("b_up", 1)
            self.go("b_up2", 1)
            self.get("b_dn", 1)
            self.go("b_dn2", 1)
        elif e == 5:
            self.get("a_pair", 3)
            self.get("a_pair", 1)
        elif e == 6:
            for i in (0, 1):
                self.get("b_up2", i)
                self.get("b_dn2", i)
        else:
            self.get("a_pair", 2)
        self.share(UNITS[e])

    def sent(self):
        for name, count in MESSAGES:
            for i in range(count):
                h, k, sent, _, part, to = self.message(name, i)
                self.copy(0, h, k, *sent, part, to).wait_send()
        for event in UNITS:
            for unit in UNITS[event]:
                self.across(0, unit).wait_send()


MESSAGES = (
    ("a_up", 1), ("a_dn", 1), ("a_up2", 1), ("a_dn2", 1), ("a_pair", 4),
    ("b_pair", 1), ("b_up", 2), ("b_dn", 2), ("b_up2", 2), ("b_dn2", 2),
)
ROUTED = 17
SWAP = 33
UNITS = {
    0: [(0, 0, 0), (1, 0, 0)],
    1: [(0, 3, 0), (0, 1, 0), (1, 0, 1)],
    2: [(1, 3, 0), (1, 1, 0), (0, 0, 1)],
    3: [(0, 2, 0)],
    4: [(1, 3, 1), (1, 1, 1)],
    5: [(0, 3, 1), (0, 1, 1)],
    6: [(1, 2, 0), (1, 2, 1)],
    7: [(0, 2, 1)],
}


class Place:
    def __init__(self):
        self.row = lax.axis_index("sa")
        self.me = lax.axis_index("an")
        self.x, self.c = self.row // CORES, self.row % CORES
        self.y, self.z = self.me // SIDE, self.me % SIDE
        self.s, self.b = self.z // PAIR, self.z % PAIR
        self.foreign = (self.c + self.s) % 2
        self.outer = self.y * SIDE + self.outer_z(self.z)
        self.mine = self.block(0, 0, 0)
        self.pair = {"sa": self.row, "an": self.y * SIDE + self.s * PAIR + 1 - self.b}
        self.twin = {"sa": self.row + 1 - 2 * self.c, "an": self.me}
        self.partner = {"sa": self.row + 1 - 2 * self.c, "an": self.outer}
        self.holder = {"sa": self.row, "an": self.outer}

    def outer_z(self, z):
        return (z + 2 * (z % PAIR) + 3) % SIDE

    def ring(self, dy):
        return {"sa": self.row, "an": ((self.y + dy) % SIDE) * SIDE + self.z}

    def block(self, lane, dy, db):
        foreign = (self.foreign + lane) % 2
        b = (self.b + db) % PAIR
        z = self.s * PAIR + b
        return ((self.y + dy) % SIDE) * SIDE + (z + foreign * (2 * b + 3)) % SIDE

    def task_of(self, an):
        y, z = an // SIDE, an % SIDE
        foreign = (self.c + z // PAIR) % 2
        return y * SIDE + (z + foreign * (2 * (z % PAIR) + 3)) % SIDE


def repeat(first, last, step):
    def one(k, carry):
        step(k)
        return carry

    lax.fori_loop(first, last, one, 0)


def either(flag, yes, no):
    pl.when(flag == 1)(yes)
    pl.when(flag == 0)(no)


def visit(own, shared, work):
    units = [(0,) + unit for unit in own] + [(1,) + unit for unit in shared]

    def one(i):
        picked = []
        for column in zip(*units):
            value = jnp.int32(column[0])
            for k in range(1, len(column)):
                value = jnp.where(i == k, jnp.int32(column[k]), value)
            picked.append(value)
        work(*picked)

    repeat(0, len(units), one)


def body(
    mine_req, table, states, w_query, w_key, w_value, w_out, enc_up, enc_down, nearby, out,
    sgat, egat, agat, wcol, wq, wkv, wrow, up, down, pool,
    wide, normed, qs, keys, vals, total, arrived, other_table, task_req, slots,
    send, recv, wsend, wrecv, lsend, lrecv, qsend, qrecv, local, wsem,
):
    p = Place()
    row, me, x, b = p.row, p.me, p.x, p.b
    tokens, width = states.shape
    wrows = w_out.shape[0] // LINE
    chunks = enc_up.shape[1] // FCHUNK
    share = x * PAIR + b

    def remote(src, dst, ssem, rsem, to):
        return pltpu.make_async_remote_copy(
            src_ref=src, dst_ref=dst, send_sem=ssem, recv_sem=rsem,
            device_id=to, device_id_type=pl.DeviceIdType.MESH,
        )

    load_states = pltpu.make_async_copy(states, sgat.at[me], local.at[0])
    stage_states = pltpu.make_async_copy(states, qs, local.at[0])
    load_rows = pltpu.make_async_copy(
        w_out.at[pl.ds(x * PAIR * wrows, PAIR * wrows)], wrow, local.at[1]
    )
    load_pool = pltpu.make_async_copy(nearby, pool, local.at[2])
    load_query = pltpu.make_async_copy(w_query, wq, local.at[3])
    load_key = pltpu.make_async_copy(w_key, wkv.at[:, pl.ds(0, width)], local.at[4])
    load_value = pltpu.make_async_copy(w_value, wkv.at[:, pl.ds(width, width)], local.at[5])
    load_column = pltpu.make_async_copy(
        w_out.at[
            pl.ds(pl.multiple_of(share * wrows, wrows), wrows),
            pl.ds(pl.multiple_of(p.mine * width, width), width),
        ],
        wcol.at[me, share],
        local.at[6],
    )

    def load_up(f):
        cut = pl.ds(pl.multiple_of(f * FCHUNK, FCHUNK), FCHUNK)
        return pltpu.make_async_copy(enc_up.at[:, cut], up.at[:, cut], wsem.at[0, f])

    def load_down(f):
        cut = pl.ds(pl.multiple_of(f * FCHUNK, FCHUNK), FCHUNK)
        return pltpu.make_async_copy(enc_down.at[cut], down.at[cut], wsem.at[1, f])

    def load_weights():
        load_key.start()
        load_value.start()
        load_query.start()

    barrier = pltpu.get_barrier_semaphore()

    def greet(to):
        pl.semaphore_signal(barrier, inc=1, device_id=to, device_id_type=pl.DeviceIdType.MESH)

    def line(k):
        far = k % PAIR
        at = far * p.outer + (1 - far) * me
        return {"sa": ((x + k // PAIR) % SIDE) * CORES + p.c, "an": at}

    greet(p.partner)
    greet(p.twin)
    repeat(1, PLANE, lambda k: greet({"sa": row, "an": (me + k) % PLANE}))
    repeat(1, LINE, lambda k: greet(line(k)))

    load_pool.start()
    repeat(0, chunks // 2, lambda f: (load_up(f).start(), load_down(f).start()))
    either(p.foreign, stage_states.start, load_states.start)
    repeat(chunks // 2, chunks, lambda f: (load_up(f).start(), load_down(f).start()))
    load_rows.start()
    load_column.start()
    pl.when(p.foreign == 0)(load_weights)

    span, own = pool.shape[1], pool.shape[0]
    requests = mine_req.shape[0]
    low, high = jnp.int32(own - 1), jnp.int32(0)
    for k in range(requests):
        offset = mine_req[k] - me * own
        here = (offset >= 0) & (offset < own)
        low = jnp.where(here, jnp.minimum(low, offset), low)
        high = jnp.where(here, jnp.maximum(high, offset), high)
    load_pool.wait()
    for slot, chosen in enumerate((low, high)):
        rows = pool[chosen].astype(F32)
        cut = pl.ds(slot * span, span)
        wide[cut] = rows
        square = jnp.mean(rows * rows, axis=-1, keepdims=True)
        normed[cut] = (rows * lax.rsqrt(square + EPS)).astype(BF16)

    def encode_chunk(f):
        load_up(f).wait()
        load_down(f).wait()
        cut = pl.ds(pl.multiple_of(f * FCHUNK, FCHUNK), FCHUNK)
        pre = jnp.dot(normed[...], up[:, cut], preferred_element_type=F32)
        hidden = (0.5 * pre * (1.0 + lax.erf(pre * 0.5**0.5))).astype(BF16)
        wide[...] += jnp.dot(hidden, down[cut], preferred_element_type=F32)

    early = 3
    repeat(0, early, encode_chunk)
    pl.semaphore_wait(barrier, PLANE - 1 + LINE - 1 + 2)

    gs = Gather(0, sgat, send, recv, p)
    ge = Gather(1, egat, send, recv, p)
    ga = Gather(2, agat, send, recv, p)

    def swap(number, h, src, buf, to_slot):
        cut = pl.ds(h * (buf.shape[1] // 2), buf.shape[1] // 2)
        return remote(
            src.at[cut], buf.at[to_slot, cut],
            send.at[number, SWAP + h], recv.at[number, SWAP + h], p.partner,
        )

    def home_states():
        load_states.wait()
        gs.own_both()

    def swap_states():
        stage_states.wait()
        for h in (0, 1):
            swap(0, h, qs, sgat, me).start()

    either(p.foreign, swap_states, home_states)
    table_copy = remote(table, other_table, qsend.at[0], qrecv.at[0], p.twin)
    table_copy.start()
    repeat(early, chunks, encode_chunk)

    def swap_encoded():
        normed[...] = wide[...].astype(BF16)
        for h in (0, 1):
            swap(1, h, normed, egat, me).start()
        for h in (0, 1):
            swap(0, h, qs, sgat, p.outer).wait_recv()
            gs.own(h)

    def keep_encoded():
        egat[me] = wide[...].astype(BF16)
        ge.own_both()

    either(p.foreign, swap_encoded, keep_encoded)

    def plane_copy(k):
        an = (me + k) % PLANE
        part = an % PAIR
        task = p.task_of(an)
        return remote(
            wrow.at[
                pl.ds(pl.multiple_of(part * wrows, wrows), wrows),
                pl.ds(pl.multiple_of(task * width, width), width),
            ],
            wcol.at[me, x * PAIR + part],
            wsend.at[k],
            wrecv.at[k],
            {"sa": row, "an": an},
        )

    def plane_arrival(k):
        ref = wcol.at[(me + PLANE - k) % PLANE, share]
        return remote(ref, ref, wsend.at[k], wrecv.at[k], {"sa": row, "an": (me + k) % PLANE})

    def line_copy(k, held):
        ref = wcol.at[:, held]
        return remote(ref, ref, lsend.at[k], lrecv.at[k], line(k))

    def line_arrival(k):
        far = k % PAIR
        part = b + far * (1 - 2 * b)
        return line_copy(k, ((x + SIDE - k // PAIR) % SIDE) * PAIR + part)

    weight_copies = (
        remote(wkv, wkv, qsend.at[1], qrecv.at[1], p.holder),
        remote(wq, wq, qsend.at[2], qrecv.at[2], p.holder),
    )

    def give_weights():
        load_key.wait()
        load_value.wait()
        load_query.wait()
        for copy in weight_copies:
            copy.start()

    def late_encoded():
        for h in (0, 1):
            swap(1, h, normed, egat, p.outer).wait_recv()
            ge.own(h)

    pl.when(p.foreign == 1)(late_encoded)
    gs.event(1)
    load_rows.wait()
    repeat(1, PLANE, lambda k: plane_copy(k).start())
    table_copy.wait_recv()
    task_copies = [
        pltpu.make_async_copy(src, task_req, local.at[7]) for src in (other_table, table)
    ]
    either(p.foreign, task_copies[0].start, task_copies[1].start)

    def find_slot(k):
        wanted = task_req[0, k]
        owner = wanted // own
        later = jnp.int32(0)
        for j in range(requests):
            other = task_req[0, j]
            later = jnp.where((other < wanted) & (other >= owner * own), jnp.int32(1), later)
        slots[k] = owner * NEIGH + later

    gs.event(2)
    pl.when(p.foreign == 0)(give_weights)
    ge.event(1)
    gs.event(3)
    ge.event(2)
    load_column.wait()
    repeat(1, PLANE, lambda k: plane_arrival(k).wait_recv())
    repeat(1, SIDE, lambda k: line_copy(PAIR * k, share).start())
    either(p.foreign, task_copies[0].wait, task_copies[1].wait)
    repeat(0, requests, find_slot)
    ge.event(3)
    pl.when(p.foreign == 1)(weight_copies[0].wait_recv)

    def project(lane, h, dy, db):
        block = p.block(lane, dy, db)
        slot = block * NEIGH + h
        cut = pl.ds(pl.multiple_of(h * span, span), span)
        both = jnp.dot(egat[block, cut], wkv[...], preferred_element_type=F32)
        keys[slot] = both[:, :width].astype(BF16)
        vals[slot] = both[:, width:].astype(BF16)

    def query_tile(t):
        cut = pl.ds(pl.multiple_of(t * 256, 256), 256)
        acc = jnp.zeros((256, width), F32)
        for j in range(PLANE):
            acc = acc + jnp.dot(
                sgat[j, cut], wq[j * width : (j + 1) * width], preferred_element_type=F32
            )
        qs[cut] = acc.astype(BF16)

    for event in range(4):
        ge.shared(event)
    early_units = UNITS[0] + UNITS[1] + UNITS[2] + UNITS[3]
    visit(early_units[:5], early_units[:5], project)
    gs.event(4)
    visit(early_units[5:], early_units[5:], project)
    ge.event(4)
    repeat(0, SIDE, lambda k: line_copy(PAIR * k + 1, share).start())
    gs.event(5)
    gs.event(6)
    gs.event(7)
    ge.shared(4)
    visit(UNITS[4], UNITS[4], project)
    ge.event(5)
    for event in UNITS:
        gs.shared(event)
    pl.when(p.foreign == 1)(weight_copies[1].wait_recv)

    def sent_states():
        for h in (0, 1):
            swap(0, h, qs, sgat, me).wait_send()

    pl.when(p.foreign == 1)(sent_states)
    repeat(0, tokens // 256, query_tile)
    ge.shared(5)
    ge.event(6)
    visit(UNITS[5] + UNITS[6], UNITS[5], project)
    ge.event(7)
    ge.shared(6)
    visit(UNITS[7], UNITS[6], project)
    ge.shared(7)
    visit([], UNITS[7], project)

    power = float(HEAD) ** -0.5 * LOG2E

    def attend(t):
        scores, held = [], []
        for g in (2 * t, 2 * t + 1):
            one, two = slots[NEIGH * g], slots[NEIGH * g + 1]
            q = qs[pl.ds(pl.multiple_of(g * GROUP, GROUP), GROUP)]
            k = jnp.concatenate([keys[one], keys[two]], axis=0)
            held.append(jnp.concatenate([vals[one], vals[two]], axis=0))
            for h in range(width // HEAD):
                part = slice(h * HEAD, (h + 1) * HEAD)
                scores.append(lax.dot_general(
                    q[:, part], k[:, part], (((1,), (1,)), ((), ())),
                    preferred_element_type=F32,
                ))
        weights = [jnp.exp2((v - jnp.max(v, axis=-1, keepdims=True)) * power) for v in scores]
        probs = [
            (w * (1.0 / jnp.sum(w, axis=-1, keepdims=True))).astype(BF16) for w in weights
        ]
        heads = width // HEAD
        rows = []
        for i in range(2):
            done = [
                jnp.dot(
                    probs[i * heads + h], held[i][:, h * HEAD : (h + 1) * HEAD],
                    preferred_element_type=F32,
                )
                for h in range(heads)
            ]
            rows.append(jnp.concatenate(done, axis=1))
        cut = pl.ds(pl.multiple_of(2 * t * GROUP, 2 * GROUP), 2 * GROUP)
        agat[p.mine, cut] = jnp.concatenate(rows, axis=0).astype(BF16)

    pairs = tokens // GROUP // 2
    repeat(0, pairs // 2, attend)
    ga.own(0)
    repeat(pairs // 2, pairs, attend)
    ga.own(1)

    total[...] = jnp.zeros_like(total)

    def add_output(lane, h, dy, db):
        j = p.block(lane, dy, db)
        cut = pl.ds(pl.multiple_of(h * half, half), half)
        total[cut] += jnp.dot(
            agat[j, cut], wcol[j].reshape(width, width), preferred_element_type=F32
        )

    half = tokens // 2

    def swap_out(h):
        cut = pl.ds(h * half, half)
        return remote(
            qs.at[cut], arrived.at[cut], send.at[2, SWAP + h], recv.at[2, SWAP + h], p.partner
        )

    def finish(h):
        cut = pl.ds(h * half, half)

        def give():
            qs[cut] = total[cut].astype(BF16)
            swap_out(h).start()

        def keep():
            out[cut] = total[cut].astype(BF16)

        either(p.foreign, give, keep)

    ga.event(1)
    ga.event(2)
    repeat(1, LINE, lambda k: line_arrival(k).wait_recv())
    ga.shared(0)
    visit(UNITS[0] + UNITS[1], UNITS[0], add_output)
    for event in (3, 4, 5):
        ga.event(event)
        ga.shared(event - 2)
        visit(UNITS[event - 1], UNITS[event - 2], add_output)
    ga.shared(4)
    visit(UNITS[5], UNITS[4], add_output)
    ga.shared(5)
    ga.event(6)
    visit(UNITS[6], UNITS[5], add_output)
    ga.shared(6)
    visit([], UNITS[6], add_output)
    finish(1)
    ga.event(7)
    visit(UNITS[7], [], add_output)
    ga.shared(7)
    visit([], UNITS[7], add_output)
    finish(0)

    def take():
        for h in (1, 0):
            cut = pl.ds(h * half, half)
            swap_out(h).wait_recv()
            out[cut] = arrived[cut]

    pl.when(p.foreign == 1)(take)

    for gather in (gs, ge, ga):
        gather.sent()
    table_copy.wait_send()

    def sent_foreign():
        for h in (0, 1):
            swap(1, h, normed, egat, me).wait_send()
            swap_out(h).wait_send()

    def sent_home():
        for copy in weight_copies:
            copy.wait_send()

    either(p.foreign, sent_foreign, sent_home)
    repeat(1, PLANE, lambda k: plane_copy(k).wait_send())
    repeat(1, LINE, lambda k: line_copy(k, share).wait_send())


def shards(
    decoder_states, w_query, w_key, w_value, w_out, enc_up, enc_down, neighbour_inputs, requests
):
    tokens, width = decoder_states.shape
    _, span, features = neighbour_inputs.shape
    hbm = pl.BlockSpec(memory_space=pl.ANY)
    slots = PLANE * NEIGH
    chunks = enc_up.shape[1] // FCHUNK
    return pl.pallas_call(
        body,
        out_shape=pltpu.VMEM((tokens, width), BF16),
        in_specs=[
            pl.BlockSpec(memory_space=pltpu.SMEM), pl.BlockSpec(memory_space=pltpu.VMEM)
        ] + [hbm] * 8,
        out_specs=pl.BlockSpec(memory_space=pltpu.VMEM),
        scratch_shapes=[
            pltpu.VMEM((PLANE, tokens, width), BF16),
            pltpu.VMEM((PLANE, NEIGH * span, features), BF16),
            pltpu.VMEM((PLANE, tokens, width), BF16),
            pltpu.VMEM((PLANE, LINE, w_out.shape[0] // LINE, width), BF16),
            pltpu.VMEM(w_query.shape, BF16),
            pltpu.VMEM((features, 2 * width), BF16),
            pltpu.VMEM((PAIR * w_out.shape[0] // LINE, w_out.shape[1]), BF16),
            pltpu.VMEM(enc_up.shape, BF16),
            pltpu.VMEM(enc_down.shape, BF16),
            pltpu.VMEM(neighbour_inputs.shape, BF16),
            pltpu.VMEM((NEIGH * span, features), F32),
            pltpu.VMEM((NEIGH * span, features), BF16),
            pltpu.VMEM((tokens, width), BF16),
            pltpu.VMEM((slots, span, width), BF16),
            pltpu.VMEM((slots, span, width), BF16),
            pltpu.VMEM((tokens, width), F32),
            pltpu.VMEM((tokens, width), BF16),
            pltpu.VMEM((1, requests.shape[0]), jnp.int32),
            pltpu.SMEM((1, requests.shape[0]), jnp.int32),
            pltpu.SMEM(requests.shape, jnp.int32),
            pltpu.SemaphoreType.DMA((3, SWAP + 2)),
            pltpu.SemaphoreType.DMA((3, SWAP + 2)),
            pltpu.SemaphoreType.DMA((PLANE,)),
            pltpu.SemaphoreType.DMA((PLANE,)),
            pltpu.SemaphoreType.DMA((LINE,)),
            pltpu.SemaphoreType.DMA((LINE,)),
            pltpu.SemaphoreType.DMA((3,)),
            pltpu.SemaphoreType.DMA((3,)),
            pltpu.SemaphoreType.DMA((8,)),
            pltpu.SemaphoreType.DMA((2, chunks)),
        ],
        compiler_params=pltpu.CompilerParams(
            collective_id=0, has_side_effects=True, vmem_limit_bytes=62 * 2**20
        ),
    )(
        requests, requests[None, :], decoder_states, w_query, w_key, w_value, w_out,
        enc_up, enc_down, neighbour_inputs,
    )


def solution(mesh):
    placed = (
        P("sa", "an"),
        P(None, "an"),
        P(None, "an"),
        P(None, "an"),
        P("an", None),
        P(),
        P(),
        P(("sa", "an"), None, None),
        P("sa"),
    )
    return jax.shard_map(
        shards, mesh=mesh, in_specs=placed, out_specs=P("sa", "an"), check_vma=False
    )
```

```python
import functools

import jax
import jax.numpy as jnp
from jax import lax
from jax.experimental import pallas as pl
from jax.experimental.pallas import tpu as pltpu
from jax.sharding import PartitionSpec as P

HEAD = 128
GROUP = 64
NEIGH = 2
EPS = 1e-06
SIDE = 4
PLANE = SIDE * SIDE
LINE = 8
FCHUNK = 512
CORES = 2
PAIR = 2
LOG2E = 1.4426950408889634
F32 = jnp.float32
BF16 = jnp.bfloat16


class Gather:
    def __init__(self, number, buf, send, recv, place, first=None):
        self.number, self.buf, self.send, self.recv = number, buf, send, recv
        self.place = place
        first = first or buf.shape[1] // 2
        self.start = (0, first)
        self.rows = (first, buf.shape[1] - first)

    def cut(self, h):
        return pl.ds(self.start[h], self.rows[h])

    def copy(self, lane, h, k, dy, db, part, to):
        rows, first = self.rows[h], self.start[h]
        if part is not None:
            rows = rows // 2
            first += part * rows
        ref = self.buf.at[self.place.block(lane, dy, db), pl.ds(first, rows)]
        return pltpu.make_async_remote_copy(
            src_ref=ref,
            dst_ref=ref,
            send_sem=self.send.at[self.number, k],
            recv_sem=self.recv.at[self.number, k],
            device_id=to,
            device_id_type=pl.DeviceIdType.MESH,
        )

    def message(self, name, i=0):
        p = self.place
        up, dn, pair = p.ring(1), p.ring(3), p.pair
        if name == "a_up":
            return 0, 0, (0, 0), (3, 0), None, up
        if name == "a_dn":
            return 0, 1, (0, 0), (1, 0), None, dn
        if name == "a_up2":
            return 0, 2, (3, 0), (2, 0), 0, up
        if name == "a_dn2":
            return 0, 3, (1, 0), (2, 0), 1, dn
        if name == "a_pair":
            return 0, 4 + i, (i, 0), (i, 1), None, pair
        if name == "b_pair":
            return 1, 8, (0, 0), (0, 1), None, pair
        if name == "b_up":
            return 1, 9 + i, (0, i), (3, i), None, up
        if name == "b_dn":
            return 1, 11 + i, (0, i), (1, i), None, dn
        if name == "b_up2":
            return 1, 13 + i, (3, i), (2, i), 0, up
        assert name == "b_dn2"
        return 1, 15 + i, (1, i), (2, i), 1, dn

    def go(self, name, i=0):
        h, k, sent, _, part, to = self.message(name, i)
        self.copy(0, h, k, *sent, part, to).start()

    def get(self, name, i=0):
        h, k, _, got, part, to = self.message(name, i)
        self.copy(0, h, k, *got, part, to).wait_recv()

    def across(self, lane, unit):
        h, dy, db = unit
        k = ROUTED + h * 8 + dy * PAIR + db
        return self.copy(lane, h, k, dy, db, None, self.place.twin)

    def share(self, units):
        for unit in units:
            self.across(0, unit).start()

    def shared(self, event):
        for unit in UNITS[event]:
            self.across(1, unit).wait_recv()

    def own(self, h):
        if h == 0:
            self.go("a_up")
            self.go("a_dn")
            self.go("a_pair", 0)
        else:
            self.go("b_pair")
            self.go("b_up", 0)
            self.go("b_dn", 0)
        self.share([UNITS[0][h]])

    def own_both(self):
        self.go("b_pair")
        self.go("a_up")
        self.go("a_dn")
        self.go("a_pair", 0)
        self.go("b_up", 0)
        self.go("b_dn", 0)
        self.share(UNITS[0])

    def event(self, e):
        if e == 1:
            self.get("a_up")
            self.go("a_up2")
            self.go("a_pair", 3)
            self.get("a_dn")
            self.go("a_dn2")
            self.go("a_pair", 1)
            self.get("b_pair")
            self.go("b_up", 1)
            self.go("b_dn", 1)
        elif e == 2:
            self.get("b_up", 0)
            self.go("b_up2", 0)
            self.get("b_dn", 0)
            self.go("b_dn2", 0)
            self.get("a_pair", 0)
        elif e == 3:
            self.get("a_up2")
            self.get("a_dn2")
            self.go("a_pair", 2)
        elif e == 4:
            self.get("b_up", 1)
            self.go("b_up2", 1)
            self.get("b_dn", 1)
            self.go("b_dn2", 1)
        elif e == 5:
            self.get("a_pair", 3)
            self.get("a_pair", 1)
        elif e in (6, 7):
            self.get("b_up2", e - 6)
            self.get("b_dn2", e - 6)
        else:
            self.get("a_pair", 2)
        self.share(UNITS[e])

    def sent(self):
        for name, count in MESSAGES:
            for i in range(count):
                h, k, sent, _, part, to = self.message(name, i)
                self.copy(0, h, k, *sent, part, to).wait_send()
        for event in UNITS:
            for unit in UNITS[event]:
                self.across(0, unit).wait_send()


MESSAGES = (
    ("a_up", 1), ("a_dn", 1), ("a_up2", 1), ("a_dn2", 1), ("a_pair", 4),
    ("b_pair", 1), ("b_up", 2), ("b_dn", 2), ("b_up2", 2), ("b_dn2", 2),
)
ROUTED = 17
SWAP = 33
UNITS = {
    0: [(0, 0, 0), (1, 0, 0)],
    1: [(0, 3, 0), (0, 1, 0), (1, 0, 1)],
    2: [(1, 3, 0), (1, 1, 0), (0, 0, 1)],
    3: [(0, 2, 0)],
    4: [(1, 3, 1), (1, 1, 1)],
    5: [(0, 3, 1), (0, 1, 1)],
    6: [(1, 2, 0)],
    7: [(1, 2, 1)],
    8: [(0, 2, 1)],
}


class Place:
    def __init__(self):
        self.row = lax.axis_index("sa")
        self.me = lax.axis_index("an")
        self.x, self.c = self.row // CORES, self.row % CORES
        self.y, self.z = self.me // SIDE, self.me % SIDE
        self.s, self.b = self.z // PAIR, self.z % PAIR
        self.foreign = (self.c + self.s) % 2
        self.outer = self.y * SIDE + self.outer_z(self.z)
        self.mine = self.block(0, 0, 0)
        self.pair = {"sa": self.row, "an": self.y * SIDE + self.s * PAIR + 1 - self.b}
        self.twin = {"sa": self.row + 1 - 2 * self.c, "an": self.me}
        self.partner = {"sa": self.row + 1 - 2 * self.c, "an": self.outer}
        self.holder = {"sa": self.row, "an": self.outer}

    def outer_z(self, z):
        return (z + 2 * (z % PAIR) + 3) % SIDE

    def ring(self, dy):
        return {"sa": self.row, "an": ((self.y + dy) % SIDE) * SIDE + self.z}

    def block(self, lane, dy, db):
        foreign = (self.foreign + lane) % 2
        b = (self.b + db) % PAIR
        z = self.s * PAIR + b
        return ((self.y + dy) % SIDE) * SIDE + (z + foreign * (2 * b + 3)) % SIDE

    def task_of(self, an):
        y, z = an // SIDE, an % SIDE
        foreign = (self.c + z // PAIR) % 2
        return y * SIDE + (z + foreign * (2 * (z % PAIR) + 3)) % SIDE


def repeat(first, last, step):
    def one(k, carry):
        step(k)
        return carry

    lax.fori_loop(first, last, one, 0)


def either(flag, yes, no):
    pl.when(flag == 1)(yes)
    pl.when(flag == 0)(no)


def visit(own, shared, work):
    for h in (0, 1):
        units = [(0,) + unit[1:] for unit in own if unit[0] == h]
        units += [(1,) + unit[1:] for unit in shared if unit[0] == h]

        def one(i):
            picked = []
            for column in zip(*units):
                value = jnp.int32(column[0])
                for k in range(1, len(column)):
                    value = jnp.where(i == k, jnp.int32(column[k]), value)
                picked.append(value)
            lane, dy, db = picked
            work(lane, h, dy, db)

        if units:
            repeat(0, len(units), one)


def body(
    mine_req, table, states, w_query, w_key, w_value, w_out, enc_up, enc_down, nearby, out,
    sgat, egat, agat, wcol, wq, wkv, wrow, up, down, pool,
    wide, normed, qs, keys, vals, total, arrived, other_table, task_req, slots,
    send, recv, wsend, wrecv, lsend, lrecv, qsend, qrecv, local, wsem,
):
    p = Place()
    row, me, x, b = p.row, p.me, p.x, p.b
    tokens, width = states.shape
    wrows = w_out.shape[0] // LINE
    chunks = enc_up.shape[1] // FCHUNK
    share = x * PAIR + b

    def remote(src, dst, ssem, rsem, to):
        return pltpu.make_async_remote_copy(
            src_ref=src, dst_ref=dst, send_sem=ssem, recv_sem=rsem,
            device_id=to, device_id_type=pl.DeviceIdType.MESH,
        )

    load_states = pltpu.make_async_copy(states, sgat.at[me], local.at[0])
    stage_states = pltpu.make_async_copy(states, qs, local.at[0])
    load_rows = pltpu.make_async_copy(
        w_out.at[pl.ds(x * PAIR * wrows, PAIR * wrows)], wrow, local.at[1]
    )
    load_pool = pltpu.make_async_copy(nearby, pool, local.at[2])
    load_query = pltpu.make_async_copy(w_query, wq, local.at[3])
    load_key = pltpu.make_async_copy(w_key, wkv.at[:, pl.ds(0, width)], local.at[4])
    load_value = pltpu.make_async_copy(w_value, wkv.at[:, pl.ds(width, width)], local.at[5])
    load_column = pltpu.make_async_copy(
        w_out.at[
            pl.ds(pl.multiple_of(share * wrows, wrows), wrows),
            pl.ds(pl.multiple_of(p.mine * width, width), width),
        ],
        wcol.at[me, share],
        local.at[6],
    )

    def load_up(f):
        cut = pl.ds(pl.multiple_of(f * FCHUNK, FCHUNK), FCHUNK)
        return pltpu.make_async_copy(enc_up.at[:, cut], up.at[:, cut], wsem.at[0, f])

    def load_down(f):
        cut = pl.ds(pl.multiple_of(f * FCHUNK, FCHUNK), FCHUNK)
        return pltpu.make_async_copy(enc_down.at[cut], down.at[cut], wsem.at[1, f])

    def load_weights():
        load_key.start()
        load_value.start()
        load_query.start()

    barrier = pltpu.get_barrier_semaphore()

    def greet(to):
        pl.semaphore_signal(barrier, inc=1, device_id=to, device_id_type=pl.DeviceIdType.MESH)

    def along(dx):
        return {"sa": ((x + dx) % SIDE) * CORES + p.c, "an": me}

    greet(p.partner)
    greet(p.twin)
    repeat(1, PLANE, lambda k: greet({"sa": row, "an": (me + k) % PLANE}))
    greet(along(1))
    greet(along(3))

    load_pool.start()
    load_rows.start()
    repeat(0, chunks // 2, lambda f: (load_up(f).start(), load_down(f).start()))
    either(p.foreign, stage_states.start, load_states.start)
    repeat(chunks // 2, chunks, lambda f: (load_up(f).start(), load_down(f).start()))
    load_column.start()
    pl.when(p.foreign == 0)(load_weights)

    span, own = pool.shape[1], pool.shape[0]
    requests = mine_req.shape[0]
    low, high = jnp.int32(own - 1), jnp.int32(0)
    for k in range(requests):
        offset = mine_req[k] - me * own
        here = (offset >= 0) & (offset < own)
        low = jnp.where(here, jnp.minimum(low, offset), low)
        high = jnp.where(here, jnp.maximum(high, offset), high)
    load_pool.wait()
    for slot, chosen in enumerate((low, high)):
        rows = pool[chosen].astype(F32)
        cut = pl.ds(slot * span, span)
        wide[cut] = rows
        square = jnp.mean(rows * rows, axis=-1, keepdims=True)
        normed[cut] = (rows * lax.rsqrt(square + EPS)).astype(BF16)

    def encode_chunk(f):
        load_up(f).wait()
        load_down(f).wait()
        cut = pl.ds(pl.multiple_of(f * FCHUNK, FCHUNK), FCHUNK)
        pre = jnp.dot(normed[...], up[:, cut], preferred_element_type=F32)
        hidden = (0.5 * pre * (1.0 + lax.erf(pre * 0.5**0.5))).astype(BF16)
        wide[...] += jnp.dot(hidden, down[cut], preferred_element_type=F32)

    early = 3
    repeat(0, early, encode_chunk)
    pl.semaphore_wait(barrier, PLANE - 1 + 4)

    gs = Gather(0, sgat, send, recv, p, first=7 * tokens // 16)
    ge = Gather(1, egat, send, recv, p)
    ga = Gather(2, agat, send, recv, p)

    def swap(gather, h, src, to_slot):
        cut, number = gather.cut(h), gather.number
        return remote(
            src.at[cut], gather.buf.at[to_slot, cut],
            send.at[number, SWAP + h], recv.at[number, SWAP + h], p.partner,
        )

    def plane_copy(k):
        an = (me + k) % PLANE
        part = an % PAIR
        task = p.task_of(an)
        return remote(
            wrow.at[
                pl.ds(pl.multiple_of(part * wrows, wrows), wrows),
                pl.ds(pl.multiple_of(task * width, width), width),
            ],
            wcol.at[me, x * PAIR + part],
            wsend.at[k],
            wrecv.at[k],
            {"sa": row, "an": an},
        )

    def home_states():
        load_states.wait()
        gs.own_both()

    def swap_states():
        stage_states.wait()
        for h in (0, 1):
            swap(gs, h, qs, me).start()

    either(p.foreign, swap_states, home_states)
    load_rows.wait()
    repeat(1, PLANE, lambda k: plane_copy(k).start())
    table_copy = remote(table, other_table, qsend.at[0], qrecv.at[0], p.twin)
    table_copy.start()
    repeat(early, chunks, encode_chunk)

    def plane_arrival(k):
        ref = wcol.at[(me + PLANE - k) % PLANE, share]
        return remote(ref, ref, wsend.at[k], wrecv.at[k], {"sa": row, "an": (me + k) % PLANE})

    def across(held):
        ref = wcol.at[:, held]
        return remote(ref, ref, lsend.at[0], lrecv.at[0], p.holder)

    def along_copy(k, held, to, part=None):
        blocks = pl.ds(0, PLANE) if part is None else pl.ds(part * (PLANE // 2), PLANE // 2)
        ref = wcol.at[blocks, pl.ds((held % SIDE) * PAIR, PAIR)]
        return remote(ref, ref, lsend.at[k], lrecv.at[k], along(to))

    def spread1():
        load_column.wait()
        repeat(1, PLANE, lambda k: plane_arrival(k).wait_recv())
        across(share).start()

    def spread2():
        across(share + 1 - 2 * b).wait_recv()
        along_copy(1, x, 1).start()
        along_copy(2, x, 3).start()

    def spread3():
        along_copy(1, x + 3, 1).wait_recv()
        along_copy(3, x + 3, 1, 0).start()
        along_copy(2, x + 1, 3).wait_recv()
        along_copy(4, x + 1, 3, 1).start()

    def spread4():
        along_copy(3, x + 2, 1, 0).wait_recv()
        along_copy(4, x + 2, 3, 1).wait_recv()

    def spread_sent():
        across(share).wait_send()
        along_copy(1, x, 1).wait_send()
        along_copy(2, x, 3).wait_send()
        along_copy(3, x, 1, 0).wait_send()
        along_copy(4, x, 3, 1).wait_send()

    def swap_encoded():
        normed[...] = wide[...].astype(BF16)
        for h in (0, 1):
            swap(ge, h, normed, me).start()
        for h in (0, 1):
            swap(gs, h, qs, p.outer).wait_recv()
            gs.own(h)

    def keep_encoded():
        egat[me] = wide[...].astype(BF16)
        ge.own_both()

    either(p.foreign, swap_encoded, keep_encoded)

    weight_copies = (
        remote(wkv, wkv, qsend.at[1], qrecv.at[1], p.holder),
        remote(wq, wq, qsend.at[2], qrecv.at[2], p.holder),
    )

    def give_weights():
        load_key.wait()
        load_value.wait()
        load_query.wait()
        for copy in weight_copies:
            copy.start()

    def late_encoded():
        for h in (0, 1):
            swap(ge, h, normed, p.outer).wait_recv()
            ge.own(h)
        spread1()

    pl.when(p.foreign == 1)(late_encoded)
    gs.event(1)
    table_copy.wait_recv()
    task_copies = [
        pltpu.make_async_copy(src, task_req, local.at[7]) for src in (other_table, table)
    ]
    either(p.foreign, task_copies[0].start, task_copies[1].start)

    def find_slot(k):
        wanted = task_req[0, k]
        owner = wanted // own
        later = jnp.int32(0)
        for j in range(requests):
            other = task_req[0, j]
            later = jnp.where((other < wanted) & (other >= owner * own), jnp.int32(1), later)
        slots[k] = owner * NEIGH + later

    def project(lane, h, dy, db):
        block = p.block(lane, dy, db)
        slot = block * NEIGH + h
        cut = pl.ds(pl.multiple_of(h * span, span), span)
        both = jnp.dot(egat[block, cut], wkv[...], preferred_element_type=F32)
        keys[slot] = both[:, :width].astype(BF16)
        vals[slot] = both[:, width:].astype(BF16)

    query_early = [u for e in range(5) for u in UNITS[e]]
    query_late = [u for e in range(5, 9) for u in UNITS[e]]

    def query_part(units, last):
        for h in (0, 1):
            blocks = [(lane, dy, db) for lane in (0, 1) for (k, dy, db) in units if k == h]
            rows = gs.rows[h] // 2

            def tile(t):
                cut = pl.ds(pl.multiple_of(gs.start[h] + t * rows, 32), rows)
                acc = total[cut] if last else jnp.zeros((rows, width), F32)
                for at in blocks:
                    j = p.block(*at)
                    acc = acc + jnp.dot(
                        sgat[j, cut], wq[pl.ds(pl.multiple_of(j * width, width), width)],
                        preferred_element_type=F32,
                    )
                if last:
                    qs[cut] = acc.astype(BF16)
                else:
                    total[cut] = acc

            repeat(0, 2, tile)

    gs.event(2)
    def spread1_then_weights():
        spread1()
        give_weights()

    either(p.foreign, spread2, spread1_then_weights)
    ge.event(1)
    gs.event(3)
    pl.when(p.foreign == 0)(spread2)
    ge.event(2)
    either(p.foreign, task_copies[0].wait, task_copies[1].wait)
    repeat(0, requests, find_slot)
    pl.when(p.foreign == 1)(weight_copies[0].wait_recv)
    visit(UNITS[0] + UNITS[1], [], project)
    ge.event(3)
    spread3()
    visit(UNITS[2] + UNITS[3], [], project)
    gs.event(4)
    for event in (0, 1):
        ge.shared(event)
    visit([], UNITS[0] + UNITS[1], project)
    ge.event(4)
    for event in (2, 3):
        ge.shared(event)
    visit(UNITS[4], UNITS[2] + UNITS[3], project)
    for event in range(5):
        gs.shared(event)

    def sent_states():
        for h in (0, 1):
            swap(gs, h, qs, me).wait_send()

    def foreign_ready():
        weight_copies[1].wait_recv()
        sent_states()

    pl.when(p.foreign == 1)(foreign_ready)
    gs.event(5)
    query_part(query_early, False)
    for event in (6, 7, 8):
        gs.event(event)
    ge.event(5)
    ge.shared(4)
    visit(UNITS[5], UNITS[4], project)
    for event in (5, 6, 7, 8):
        gs.shared(event)
    for event in (6, 7, 8):
        ge.event(event)
    query_part(query_late, True)
    ge.shared(5)
    ge.shared(6)
    visit(UNITS[6] + UNITS[7] + UNITS[8], UNITS[5] + UNITS[6], project)
    ge.shared(7)
    ge.shared(8)
    visit([], UNITS[7] + UNITS[8], project)

    power = float(HEAD) ** -0.5 * LOG2E

    def attend(t):
        scores, held = [], []
        for g in (2 * t, 2 * t + 1):
            one, two = slots[NEIGH * g], slots[NEIGH * g + 1]
            q = qs[pl.ds(pl.multiple_of(g * GROUP, GROUP), GROUP)]
            k = jnp.concatenate([keys[one], keys[two]], axis=0)
            held.append(jnp.concatenate([vals[one], vals[two]], axis=0))
            for h in range(width // HEAD):
                part = slice(h * HEAD, (h + 1) * HEAD)
                scores.append(lax.dot_general(
                    q[:, part], k[:, part], (((1,), (1,)), ((), ())),
                    preferred_element_type=F32,
                ))
        weights = [jnp.exp2((v - jnp.max(v, axis=-1, keepdims=True)) * power) for v in scores]
        probs = [
            (w * (1.0 / jnp.sum(w, axis=-1, keepdims=True))).astype(BF16) for w in weights
        ]
        heads = width // HEAD
        rows = []
        for i in range(2):
            done = [
                jnp.dot(
                    probs[i * heads + h], held[i][:, h * HEAD : (h + 1) * HEAD],
                    preferred_element_type=F32,
                )
                for h in range(heads)
            ]
            rows.append(jnp.concatenate(done, axis=1))
        cut = pl.ds(pl.multiple_of(2 * t * GROUP, 2 * GROUP), 2 * GROUP)
        agat[p.mine, cut] = jnp.concatenate(rows, axis=0).astype(BF16)

    pairs = tokens // GROUP // 2
    repeat(0, pairs // 2, attend)
    ga.own(0)
    repeat(pairs // 2, pairs, attend)
    ga.own(1)

    total[...] = jnp.zeros_like(total)

    def add_output(lane, h, dy, db):
        j = p.block(lane, dy, db)
        cut = pl.ds(pl.multiple_of(h * half, half), half)
        total[cut] += jnp.dot(
            agat[j, cut], wcol[j].reshape(width, width), preferred_element_type=F32
        )

    half = tokens // 2

    def swap_out(h):
        cut = pl.ds(h * half, half)
        return remote(
            qs.at[cut], arrived.at[cut], send.at[2, SWAP + h], recv.at[2, SWAP + h], p.partner
        )

    def finish(h):
        cut = pl.ds(h * half, half)

        def give():
            qs[cut] = total[cut].astype(BF16)
            swap_out(h).start()

        def keep():
            out[cut] = total[cut].astype(BF16)

        either(p.foreign, give, keep)

    ga.event(1)
    ga.event(2)
    spread4()
    ga.shared(0)
    visit(UNITS[0] + UNITS[1], UNITS[0], add_output)
    for event in (3, 4):
        ga.event(event)
        ga.shared(event - 2)
        visit(UNITS[event - 1], UNITS[event - 2], add_output)
    ga.shared(3)
    visit(UNITS[4], UNITS[3], add_output)
    ga.event(5)
    ga.event(6)
    ga.shared(4)
    visit(UNITS[5] + UNITS[6], UNITS[4], add_output)
    ga.event(7)
    ga.shared(5)
    ga.shared(6)
    visit(UNITS[7], UNITS[5] + UNITS[6], add_output)
    ga.shared(7)
    visit([], UNITS[7], add_output)
    finish(1)
    ga.event(8)
    visit(UNITS[8], [], add_output)
    ga.shared(8)
    visit([], UNITS[8], add_output)
    finish(0)

    def take():
        for h in (1, 0):
            cut = pl.ds(h * half, half)
            swap_out(h).wait_recv()
            out[cut] = arrived[cut]

    pl.when(p.foreign == 1)(take)

    for gather in (gs, ge, ga):
        gather.sent()
    table_copy.wait_send()

    def sent_foreign():
        for h in (0, 1):
            swap(ge, h, normed, me).wait_send()
            swap_out(h).wait_send()

    def sent_home():
        for copy in weight_copies:
            copy.wait_send()

    either(p.foreign, sent_foreign, sent_home)
    repeat(1, PLANE, lambda k: plane_copy(k).wait_send())
    spread_sent()


def shards(
    decoder_states, w_query, w_key, w_value, w_out, enc_up, enc_down, neighbour_inputs, requests
):
    tokens, width = decoder_states.shape
    _, span, features = neighbour_inputs.shape
    hbm = pl.BlockSpec(memory_space=pl.ANY)
    slots = PLANE * NEIGH
    chunks = enc_up.shape[1] // FCHUNK
    return pl.pallas_call(
        body,
        out_shape=pltpu.VMEM((tokens, width), BF16),
        in_specs=[
            pl.BlockSpec(memory_space=pltpu.SMEM), pl.BlockSpec(memory_space=pltpu.VMEM)
        ] + [hbm] * 8,
        out_specs=pl.BlockSpec(memory_space=pltpu.VMEM),
        scratch_shapes=[
            pltpu.VMEM((PLANE, tokens, width), BF16),
            pltpu.VMEM((PLANE, NEIGH * span, features), BF16),
            pltpu.VMEM((PLANE, tokens, width), BF16),
            pltpu.VMEM((PLANE, LINE, w_out.shape[0] // LINE, width), BF16),
            pltpu.VMEM(w_query.shape, BF16),
            pltpu.VMEM((features, 2 * width), BF16),
            pltpu.VMEM((PAIR * w_out.shape[0] // LINE, w_out.shape[1]), BF16),
            pltpu.VMEM(enc_up.shape, BF16),
            pltpu.VMEM(enc_down.shape, BF16),
            pltpu.VMEM(neighbour_inputs.shape, BF16),
            pltpu.VMEM((NEIGH * span, features), F32),
            pltpu.VMEM((NEIGH * span, features), BF16),
            pltpu.VMEM((tokens, width), BF16),
            pltpu.VMEM((slots, span, width), BF16),
            pltpu.VMEM((slots, span, width), BF16),
            pltpu.VMEM((tokens, width), F32),
            pltpu.VMEM((tokens, width), BF16),
            pltpu.VMEM((1, requests.shape[0]), jnp.int32),
            pltpu.SMEM((1, requests.shape[0]), jnp.int32),
            pltpu.SMEM(requests.shape, jnp.int32),
            pltpu.SemaphoreType.DMA((3, SWAP + 2)),
            pltpu.SemaphoreType.DMA((3, SWAP + 2)),
            pltpu.SemaphoreType.DMA((PLANE,)),
            pltpu.SemaphoreType.DMA((PLANE,)),
            pltpu.SemaphoreType.DMA((5,)),
            pltpu.SemaphoreType.DMA((5,)),
            pltpu.SemaphoreType.DMA((3,)),
            pltpu.SemaphoreType.DMA((3,)),
            pltpu.SemaphoreType.DMA((8,)),
            pltpu.SemaphoreType.DMA((2, chunks)),
        ],
        compiler_params=pltpu.CompilerParams(
            collective_id=0, has_side_effects=True, vmem_limit_bytes=62 * 2**20
        ),
    )(
        requests, requests[None, :], decoder_states, w_query, w_key, w_value, w_out,
        enc_up, enc_down, neighbour_inputs,
    )


def solution(mesh):
    placed = (
        P("sa", "an"),
        P(None, "an"),
        P(None, "an"),
        P(None, "an"),
        P("an", None),
        P(),
        P(),
        P(("sa", "an"), None, None),
        P("sa"),
    )
    return jax.shard_map(
        shards, mesh=mesh, in_specs=placed, out_specs=P("sa", "an"), check_vma=False
    )
```

```python
import functools

import jax
import jax.numpy as jnp
from jax import lax
from jax.experimental import pallas as pl
from jax.experimental.pallas import tpu as pltpu
from jax.sharding import PartitionSpec as P

HEAD = 128
GROUP = 64
NEIGH = 2
EPS = 1e-06
SIDE = 4
PLANE = SIDE * SIDE
LINE = 8
FCHUNK = 512
CORES = 2
PAIR = 2
LOG2E = 1.4426950408889634
F32 = jnp.float32
BF16 = jnp.bfloat16


class Gather:
    def __init__(self, number, buf, send, recv, place, first=None):
        self.number, self.buf, self.send, self.recv = number, buf, send, recv
        self.place = place
        first = first or buf.shape[1] // 2
        self.start = (0, first)
        self.rows = (first, buf.shape[1] - first)

    def cut(self, h):
        return pl.ds(self.start[h], self.rows[h])

    def copy(self, lane, h, k, dy, db, part, to):
        rows, first = self.rows[h], self.start[h]
        if part is not None:
            rows = rows // 2
            first += part * rows
        ref = self.buf.at[self.place.block(lane, dy, db), pl.ds(first, rows)]
        return pltpu.make_async_remote_copy(
            src_ref=ref,
            dst_ref=ref,
            send_sem=self.send.at[self.number],
            recv_sem=self.recv.at[self.number, k],
            device_id=to,
            device_id_type=pl.DeviceIdType.MESH,
        )

    def message(self, name, i=0):
        p = self.place
        up, dn, pair = p.ring(1), p.ring(3), p.pair
        if name == "a_up":
            return 0, 0, (0, 0), (3, 0), None, up
        if name == "a_dn":
            return 0, 1, (0, 0), (1, 0), None, dn
        if name == "a_up2":
            return 0, 2, (3, 0), (2, 0), 0, up
        if name == "a_dn2":
            return 0, 3, (1, 0), (2, 0), 1, dn
        if name == "a_pair":
            return 0, 4 + i, (i, 0), (i, 1), None, pair
        if name == "b_pair":
            return 1, 8, (0, 0), (0, 1), None, pair
        if name == "b_up":
            return 1, 9 + i, (0, i), (3, i), None, up
        if name == "b_dn":
            return 1, 11 + i, (0, i), (1, i), None, dn
        if name == "b_up2":
            return 1, 13 + i, (3, i), (2, i), 0, up
        assert name == "b_dn2"
        return 1, 15 + i, (1, i), (2, i), 1, dn

    def go(self, name, i=0):
        h, k, sent, _, part, to = self.message(name, i)
        self.copy(0, h, k, *sent, part, to).start()

    def get(self, name, i=0):
        h, k, _, got, part, to = self.message(name, i)
        self.copy(0, h, k, *got, part, to).wait_recv()

    def across(self, lane, unit):
        h, dy, db = unit
        k = ROUTED + h * 8 + dy * PAIR + db
        return self.copy(lane, h, k, dy, db, None, self.place.twin)

    def share(self, units):
        for unit in units:
            self.across(0, unit).start()

    def shared(self, event):
        for unit in UNITS[event]:
            self.across(1, unit).wait_recv()

    def own(self, h):
        if h == 0:
            self.go("a_up")
            self.go("a_dn")
            self.go("a_pair", 0)
        else:
            self.go("b_pair")
            self.go("b_up", 0)
            self.go("b_dn", 0)
        self.share([UNITS[0][h]])

    def own_both(self):
        self.go("b_pair")
        self.go("a_up")
        self.go("a_dn")
        self.go("a_pair", 0)
        self.go("b_up", 0)
        self.go("b_dn", 0)
        self.share(UNITS[0])

    def event(self, e):
        if e == 1:
            self.get("a_up")
            self.go("a_up2")
            self.go("a_pair", 3)
            self.get("a_dn")
            self.go("a_dn2")
            self.go("a_pair", 1)
            self.get("b_pair")
            self.go("b_up", 1)
            self.go("b_dn", 1)
        elif e == 2:
            self.get("b_up", 0)
            self.go("b_up2", 0)
            self.get("b_dn", 0)
            self.go("b_dn2", 0)
            self.get("a_pair", 0)
        elif e == 3:
            self.get("a_up2")
            self.get("a_dn2")
            self.go("a_pair", 2)
        elif e == 4:
            self.get("b_up", 1)
            self.go("b_up2", 1)
            self.get("b_dn", 1)
            self.go("b_dn2", 1)
        elif e == 5:
            self.get("a_pair", 3)
            self.get("a_pair", 1)
        elif e in (6, 7):
            self.get("b_up2", e - 6)
            self.get("b_dn2", e - 6)
        else:
            self.get("a_pair", 2)
        self.share(UNITS[e])

    def sent(self):
        ref = self.buf.at[pl.ds(0, PLANE - 1)]
        pltpu.make_async_remote_copy(
            src_ref=ref, dst_ref=ref, send_sem=self.send.at[self.number],
            recv_sem=self.recv.at[self.number, 0], device_id=self.place.pair,
            device_id_type=pl.DeviceIdType.MESH,
        ).wait_send()


ROUTED = 17
SWAP = 33
UNITS = {
    0: [(0, 0, 0), (1, 0, 0)],
    1: [(0, 3, 0), (0, 1, 0), (1, 0, 1)],
    2: [(1, 3, 0), (1, 1, 0), (0, 0, 1)],
    3: [(0, 2, 0)],
    4: [(1, 3, 1), (1, 1, 1)],
    5: [(0, 3, 1), (0, 1, 1)],
    6: [(1, 2, 0)],
    7: [(1, 2, 1)],
    8: [(0, 2, 1)],
}


class Place:
    def __init__(self):
        self.row = lax.axis_index("sa")
        self.me = lax.axis_index("an")
        self.x, self.c = self.row // CORES, self.row % CORES
        self.y, self.z = self.me // SIDE, self.me % SIDE
        self.s, self.b = self.z // PAIR, self.z % PAIR
        self.foreign = (self.c + self.s) % 2
        self.outer = self.y * SIDE + self.outer_z(self.z)
        self.mine = self.block(0, 0, 0)
        self.pair = {"sa": self.row, "an": self.y * SIDE + self.s * PAIR + 1 - self.b}
        self.twin = {"sa": self.row + 1 - 2 * self.c, "an": self.me}
        self.partner = {"sa": self.row + 1 - 2 * self.c, "an": self.outer}
        self.holder = {"sa": self.row, "an": self.outer}

    def outer_z(self, z):
        return (z + 2 * (z % PAIR) + 3) % SIDE

    def ring(self, dy):
        return {"sa": self.row, "an": ((self.y + dy) % SIDE) * SIDE + self.z}

    def block(self, lane, dy, db):
        foreign = (self.foreign + lane) % 2
        b = (self.b + db) % PAIR
        z = self.s * PAIR + b
        return ((self.y + dy) % SIDE) * SIDE + (z + foreign * (2 * b + 3)) % SIDE

    def task_of(self, an):
        y, z = an // SIDE, an % SIDE
        foreign = (self.c + z // PAIR) % 2
        return y * SIDE + (z + foreign * (2 * (z % PAIR) + 3)) % SIDE


def repeat(first, last, step):
    def one(k, carry):
        step(k)
        return carry

    lax.fori_loop(first, last, one, 0)


def either(flag, yes, no):
    pl.when(flag == 1)(yes)
    pl.when(flag == 0)(no)


def visit(own, shared, work):
    for h in (0, 1):
        units = [(0,) + unit[1:] for unit in own if unit[0] == h]
        units += [(1,) + unit[1:] for unit in shared if unit[0] == h]

        def one(i):
            picked = []
            for column in zip(*units):
                value = jnp.int32(column[0])
                for k in range(1, len(column)):
                    value = jnp.where(i == k, jnp.int32(column[k]), value)
                picked.append(value)
            lane, dy, db = picked
            work(lane, h, dy, db)

        if units:
            repeat(0, len(units), one)


def body(
    mine_req, table, states, w_query, w_key, w_value, w_out, enc_up, enc_down, nearby, out,
    sgat, egat, agat, wcol, wq, wkv, wrow, up, down, pool,
    wide, normed, qs, keys, vals, total, arrived, other_table, task_req, slots,
    send, swapped, recv, wsend, wrecv, lsend, lrecv, qsend, qrecv, local, wsem,
):
    p = Place()
    row, me, x, b = p.row, p.me, p.x, p.b
    tokens, width = states.shape
    wrows = w_out.shape[0] // LINE
    chunks = enc_up.shape[1] // FCHUNK
    share = x * PAIR + b

    def remote(src, dst, ssem, rsem, to):
        return pltpu.make_async_remote_copy(
            src_ref=src, dst_ref=dst, send_sem=ssem, recv_sem=rsem,
            device_id=to, device_id_type=pl.DeviceIdType.MESH,
        )

    load_states = pltpu.make_async_copy(states, sgat.at[me], local.at[0])
    stage_states = pltpu.make_async_copy(states, qs, local.at[0])
    load_rows = pltpu.make_async_copy(
        w_out.at[pl.ds(x * PAIR * wrows, PAIR * wrows)], wrow, local.at[1]
    )
    load_pool = pltpu.make_async_copy(nearby, pool, local.at[2])
    load_query = pltpu.make_async_copy(w_query, wq, local.at[3])
    load_key = pltpu.make_async_copy(w_key, wkv.at[:, pl.ds(0, width)], local.at[4])
    load_value = pltpu.make_async_copy(w_value, wkv.at[:, pl.ds(width, width)], local.at[5])
    load_column = pltpu.make_async_copy(
        w_out.at[
            pl.ds(pl.multiple_of(share * wrows, wrows), wrows),
            pl.ds(pl.multiple_of(p.mine * width, width), width),
        ],
        wcol.at[me, share],
        local.at[6],
    )

    def load_up(f):
        cut = pl.ds(pl.multiple_of(f * FCHUNK, FCHUNK), FCHUNK)
        return pltpu.make_async_copy(enc_up.at[:, cut], up.at[:, cut], wsem.at[0, f])

    def load_down(f):
        cut = pl.ds(pl.multiple_of(f * FCHUNK, FCHUNK), FCHUNK)
        return pltpu.make_async_copy(enc_down.at[cut], down.at[cut], wsem.at[1, f])

    def load_weights():
        load_key.start()
        load_value.start()
        load_query.start()

    barrier = pltpu.get_barrier_semaphore()

    def greet(to):
        pl.semaphore_signal(barrier, inc=1, device_id=to, device_id_type=pl.DeviceIdType.MESH)

    def along(dx):
        return {"sa": ((x + dx) % SIDE) * CORES + p.c, "an": me}

    greet(p.partner)
    greet(p.twin)
    repeat(1, PLANE, lambda k: greet({"sa": row, "an": (me + k) % PLANE}))
    greet(along(1))
    greet(along(3))

    load_pool.start()
    load_rows.start()
    repeat(0, chunks // 2, lambda f: (load_up(f).start(), load_down(f).start()))
    either(p.foreign, stage_states.start, load_states.start)
    repeat(chunks // 2, chunks, lambda f: (load_up(f).start(), load_down(f).start()))
    load_column.start()
    pl.when(p.foreign == 0)(load_weights)

    span, own = pool.shape[1], pool.shape[0]
    requests = mine_req.shape[0]
    low, high = jnp.int32(own - 1), jnp.int32(0)
    for k in range(requests):
        offset = mine_req[k] - me * own
        here = (offset >= 0) & (offset < own)
        low = jnp.where(here, jnp.minimum(low, offset), low)
        high = jnp.where(here, jnp.maximum(high, offset), high)
    load_pool.wait()
    for slot, chosen in enumerate((low, high)):
        rows = pool[chosen].astype(F32)
        cut = pl.ds(slot * span, span)
        wide[cut] = rows
        square = jnp.mean(rows * rows, axis=-1, keepdims=True)
        normed[cut] = (rows * lax.rsqrt(square + EPS)).astype(BF16)

    def encode_chunk(f):
        load_up(f).wait()
        load_down(f).wait()
        cut = pl.ds(pl.multiple_of(f * FCHUNK, FCHUNK), FCHUNK)
        pre = jnp.dot(normed[...], up[:, cut], preferred_element_type=F32)
        hidden = (0.5 * pre * (1.0 + lax.erf(pre * 0.5**0.5))).astype(BF16)
        wide[...] += jnp.dot(hidden, down[cut], preferred_element_type=F32)

    early = 3
    repeat(0, early, encode_chunk)
    pl.semaphore_wait(barrier, PLANE - 1 + 4)

    gs = Gather(0, sgat, send, recv, p, first=7 * tokens // 16)
    ge = Gather(1, egat, send, recv, p)
    ga = Gather(2, agat, send, recv, p)

    def swap(gather, h, src, to_slot):
        cut, number = gather.cut(h), gather.number
        return remote(
            src.at[cut], gather.buf.at[to_slot, cut],
            swapped.at[number, h], recv.at[number, SWAP + h], p.partner,
        )

    def plane_copy(k):
        an = (me + k) % PLANE
        part = an % PAIR
        task = p.task_of(an)
        return remote(
            wrow.at[
                pl.ds(pl.multiple_of(part * wrows, wrows), wrows),
                pl.ds(pl.multiple_of(task * width, width), width),
            ],
            wcol.at[me, x * PAIR + part],
            wsend.at[0],
            wrecv.at[0],
            {"sa": row, "an": an},
        )

    def home_states():
        load_states.wait()
        gs.own_both()

    def swap_states():
        stage_states.wait()
        for h in (0, 1):
            swap(gs, h, qs, me).start()

    either(p.foreign, swap_states, home_states)
    load_rows.wait()
    repeat(1, PLANE, lambda k: plane_copy(k).start())
    table_copy = remote(table, other_table, qsend.at[0], qrecv.at[0], p.twin)
    table_copy.start()
    repeat(early, chunks, encode_chunk)

    def plane_all():
        ref = wcol.at[pl.ds(0, PLANE - 1), share]
        return remote(ref, ref, wsend.at[0], wrecv.at[0], p.pair)

    def across(held):
        ref = wcol.at[:, held]
        return remote(ref, ref, lsend.at[0], lrecv.at[0], p.holder)

    def along_copy(k, held, to, part=None):
        blocks = pl.ds(0, PLANE) if part is None else pl.ds(part * (PLANE // 2), PLANE // 2)
        ref = wcol.at[blocks, pl.ds((held % SIDE) * PAIR, PAIR)]
        return remote(ref, ref, lsend.at[k], lrecv.at[k], along(to))

    def spread1():
        load_column.wait()
        plane_all().wait_recv()
        across(share).start()

    def spread2():
        across(share + 1 - 2 * b).wait_recv()
        along_copy(1, x, 1).start()
        along_copy(2, x, 3).start()

    def spread3():
        along_copy(1, x + 3, 1).wait_recv()
        along_copy(3, x + 3, 1, 0).start()
        along_copy(2, x + 1, 3).wait_recv()
        along_copy(4, x + 1, 3, 1).start()

    def spread4():
        along_copy(3, x + 2, 1, 0).wait_recv()
        along_copy(4, x + 2, 3, 1).wait_recv()

    def spread_sent():
        across(share).wait_send()
        along_copy(1, x, 1).wait_send()
        along_copy(2, x, 3).wait_send()
        along_copy(3, x, 1, 0).wait_send()
        along_copy(4, x, 3, 1).wait_send()

    def swap_encoded():
        normed[...] = wide[...].astype(BF16)
        for h in (0, 1):
            swap(ge, h, normed, me).start()
        for h in (0, 1):
            swap(gs, h, qs, p.outer).wait_recv()
            gs.own(h)

    def keep_encoded():
        egat[me] = wide[...].astype(BF16)
        ge.own_both()

    either(p.foreign, swap_encoded, keep_encoded)

    weight_copies = (
        remote(wkv, wkv, qsend.at[1], qrecv.at[1], p.holder),
        remote(wq, wq, qsend.at[2], qrecv.at[2], p.holder),
    )

    def give_weights():
        load_key.wait()
        load_value.wait()
        load_query.wait()
        for copy in weight_copies:
            copy.start()

    def late_encoded():
        for h in (0, 1):
            swap(ge, h, normed, p.outer).wait_recv()
            ge.own(h)
        spread1()

    pl.when(p.foreign == 1)(late_encoded)
    gs.event(1)
    table_copy.wait_recv()
    task_copies = [
        pltpu.make_async_copy(src, task_req, local.at[7]) for src in (other_table, table)
    ]
    either(p.foreign, task_copies[0].start, task_copies[1].start)

    def find_slot(k):
        wanted = task_req[0, k]
        owner = wanted // own
        later = jnp.int32(0)
        for j in range(requests):
            other = task_req[0, j]
            later = jnp.where((other < wanted) & (other >= owner * own), jnp.int32(1), later)
        slots[k] = owner * NEIGH + later

    def project(lane, h, dy, db):
        block = p.block(lane, dy, db)
        slot = block * NEIGH + h
        cut = pl.ds(pl.multiple_of(h * span, span), span)
        both = jnp.dot(egat[block, cut], wkv[...], preferred_element_type=F32)
        keys[slot] = both[:, :width].astype(BF16)
        vals[slot] = both[:, width:].astype(BF16)

    query_early = [u for e in range(5) for u in UNITS[e]]
    query_late = [u for e in range(5, 9) for u in UNITS[e]]

    def query_part(units, last):
        for h in (0, 1):
            blocks = [(lane, dy, db) for lane in (0, 1) for (k, dy, db) in units if k == h]
            rows = gs.rows[h] // 2

            def tile(t):
                cut = pl.ds(pl.multiple_of(gs.start[h] + t * rows, 32), rows)
                acc = total[cut] if last else jnp.zeros((rows, width), F32)
                for at in blocks:
                    j = p.block(*at)
                    acc = acc + jnp.dot(
                        sgat[j, cut], wq[pl.ds(pl.multiple_of(j * width, width), width)],
                        preferred_element_type=F32,
                    )
                if last:
                    qs[cut] = acc.astype(BF16)
                else:
                    total[cut] = acc

            repeat(0, 2, tile)

    gs.event(2)
    def spread1_then_weights():
        spread1()
        give_weights()

    either(p.foreign, spread2, spread1_then_weights)
    ge.event(1)
    gs.event(3)
    pl.when(p.foreign == 0)(spread2)
    ge.event(2)
    either(p.foreign, task_copies[0].wait, task_copies[1].wait)
    repeat(0, requests, find_slot)
    pl.when(p.foreign == 1)(weight_copies[0].wait_recv)
    visit(UNITS[0] + UNITS[1], [], project)
    ge.event(3)
    spread3()
    visit(UNITS[2] + UNITS[3], [], project)
    gs.event(4)
    for event in (0, 1):
        ge.shared(event)
    visit([], UNITS[0] + UNITS[1], project)
    ge.event(4)
    for event in (2, 3):
        ge.shared(event)
    visit(UNITS[4], UNITS[2] + UNITS[3], project)
    for event in range(5):
        gs.shared(event)

    def sent_states():
        for h in (0, 1):
            swap(gs, h, qs, me).wait_send()

    def foreign_ready():
        weight_copies[1].wait_recv()
        sent_states()

    gs.event(5)
    pl.when(p.foreign == 1)(foreign_ready)
    query_part(query_early, False)
    for event in (6, 7, 8):
        gs.event(event)
    ge.event(5)
    ge.shared(4)
    visit(UNITS[5], UNITS[4], project)
    for event in (5, 6, 7, 8):
        gs.shared(event)
    for event in (6, 7, 8):
        ge.event(event)
    query_part(query_late, True)
    ge.shared(5)
    ge.shared(6)
    visit(UNITS[6] + UNITS[7] + UNITS[8], UNITS[5] + UNITS[6], project)
    ge.shared(7)
    ge.shared(8)
    visit([], UNITS[7] + UNITS[8], project)

    power = float(HEAD) ** -0.5 * LOG2E

    def attend(t):
        scores, held = [], []
        for g in (2 * t, 2 * t + 1):
            one, two = slots[NEIGH * g], slots[NEIGH * g + 1]
            q = qs[pl.ds(pl.multiple_of(g * GROUP, GROUP), GROUP)]
            k = jnp.concatenate([keys[one], keys[two]], axis=0)
            held.append(jnp.concatenate([vals[one], vals[two]], axis=0))
            for h in range(width // HEAD):
                part = slice(h * HEAD, (h + 1) * HEAD)
                scores.append(lax.dot_general(
                    q[:, part], k[:, part], (((1,), (1,)), ((), ())),
                    preferred_element_type=F32,
                ))
        weights = [jnp.exp2((v - jnp.max(v, axis=-1, keepdims=True)) * power) for v in scores]
        probs = [
            (w * (1.0 / jnp.sum(w, axis=-1, keepdims=True))).astype(BF16) for w in weights
        ]
        heads = width // HEAD
        rows = []
        for i in range(2):
            done = [
                jnp.dot(
                    probs[i * heads + h], held[i][:, h * HEAD : (h + 1) * HEAD],
                    preferred_element_type=F32,
                )
                for h in range(heads)
            ]
            rows.append(jnp.concatenate(done, axis=1))
        cut = pl.ds(pl.multiple_of(2 * t * GROUP, 2 * GROUP), 2 * GROUP)
        agat[p.mine, cut] = jnp.concatenate(rows, axis=0).astype(BF16)

    pairs = tokens // GROUP // 2
    repeat(0, pairs // 2, attend)
    ga.own(0)
    repeat(pairs // 2, pairs, attend)
    ga.own(1)

    total[...] = jnp.zeros_like(total)

    def add_output(lane, h, dy, db):
        j = p.block(lane, dy, db)
        cut = pl.ds(pl.multiple_of(h * half, half), half)
        total[cut] += jnp.dot(
            agat[j, cut], wcol[j].reshape(width, width), preferred_element_type=F32
        )

    half = tokens // 2

    def swap_out(h):
        cut = pl.ds(h * half, half)
        return remote(
            qs.at[cut], arrived.at[cut], swapped.at[2, h], recv.at[2, SWAP + h], p.partner
        )

    def finish(h):
        cut = pl.ds(h * half, half)

        def give():
            qs[cut] = total[cut].astype(BF16)
            swap_out(h).start()

        def keep():
            out[cut] = total[cut].astype(BF16)

        either(p.foreign, give, keep)

    ga.event(1)
    ga.event(2)
    spread4()
    ga.shared(0)
    visit(UNITS[0] + UNITS[1], UNITS[0], add_output)
    for event in (3, 4):
        ga.event(event)
        ga.shared(event - 2)
        visit(UNITS[event - 1], UNITS[event - 2], add_output)
    ga.shared(3)
    visit(UNITS[4], UNITS[3], add_output)
    ga.event(5)
    ga.event(6)
    ga.shared(4)
    visit(UNITS[5] + UNITS[6], UNITS[4], add_output)
    ga.event(7)
    ga.shared(5)
    ga.shared(6)
    visit(UNITS[7], UNITS[5] + UNITS[6], add_output)
    ga.shared(7)
    visit([], UNITS[7], add_output)
    finish(1)
    ga.event(8)
    visit(UNITS[8], [], add_output)
    ga.shared(8)
    visit([], UNITS[8], add_output)
    finish(0)

    def take():
        for h in (1, 0):
            cut = pl.ds(h * half, half)
            swap_out(h).wait_recv()
            out[cut] = arrived[cut]

    pl.when(p.foreign == 1)(take)

    for gather in (gs, ge, ga):
        gather.sent()
    table_copy.wait_send()

    def sent_foreign():
        for h in (0, 1):
            swap(ge, h, normed, me).wait_send()
            swap_out(h).wait_send()

    def sent_home():
        for copy in weight_copies:
            copy.wait_send()

    either(p.foreign, sent_foreign, sent_home)
    plane_all().wait_send()
    spread_sent()


def shards(
    decoder_states, w_query, w_key, w_value, w_out, enc_up, enc_down, neighbour_inputs, requests
):
    tokens, width = decoder_states.shape
    _, span, features = neighbour_inputs.shape
    hbm = pl.BlockSpec(memory_space=pl.ANY)
    slots = PLANE * NEIGH
    chunks = enc_up.shape[1] // FCHUNK
    return pl.pallas_call(
        body,
        out_shape=pltpu.VMEM((tokens, width), BF16),
        in_specs=[
            pl.BlockSpec(memory_space=pltpu.SMEM), pl.BlockSpec(memory_space=pltpu.VMEM)
        ] + [hbm] * 8,
        out_specs=pl.BlockSpec(memory_space=pltpu.VMEM),
        scratch_shapes=[
            pltpu.VMEM((PLANE, tokens, width), BF16),
            pltpu.VMEM((PLANE, NEIGH * span, features), BF16),
            pltpu.VMEM((PLANE, tokens, width), BF16),
            pltpu.VMEM((PLANE, LINE, w_out.shape[0] // LINE, width), BF16),
            pltpu.VMEM(w_query.shape, BF16),
            pltpu.VMEM((features, 2 * width), BF16),
            pltpu.VMEM((PAIR * w_out.shape[0] // LINE, w_out.shape[1]), BF16),
            pltpu.VMEM(enc_up.shape, BF16),
            pltpu.VMEM(enc_down.shape, BF16),
            pltpu.VMEM(neighbour_inputs.shape, BF16),
            pltpu.VMEM((NEIGH * span, features), F32),
            pltpu.VMEM((NEIGH * span, features), BF16),
            pltpu.VMEM((tokens, width), BF16),
            pltpu.VMEM((slots, span, width), BF16),
            pltpu.VMEM((slots, span, width), BF16),
            pltpu.VMEM((tokens, width), F32),
            pltpu.VMEM((tokens, width), BF16),
            pltpu.VMEM((1, requests.shape[0]), jnp.int32),
            pltpu.SMEM((1, requests.shape[0]), jnp.int32),
            pltpu.SMEM(requests.shape, jnp.int32),
            pltpu.SemaphoreType.DMA((3,)),
            pltpu.SemaphoreType.DMA((3, 2)),
            pltpu.SemaphoreType.DMA((3, SWAP + 2)),
            pltpu.SemaphoreType.DMA((1,)),
            pltpu.SemaphoreType.DMA((1,)),
            pltpu.SemaphoreType.DMA((5,)),
            pltpu.SemaphoreType.DMA((5,)),
            pltpu.SemaphoreType.DMA((3,)),
            pltpu.SemaphoreType.DMA((3,)),
            pltpu.SemaphoreType.DMA((8,)),
            pltpu.SemaphoreType.DMA((2, chunks)),
        ],
        compiler_params=pltpu.CompilerParams(
            collective_id=0, has_side_effects=True, vmem_limit_bytes=62 * 2**20
        ),
    )(
        requests, requests[None, :], decoder_states, w_query, w_key, w_value, w_out,
        enc_up, enc_down, neighbour_inputs,
    )


def solution(mesh):
    placed = (
        P("sa", "an"),
        P(None, "an"),
        P(None, "an"),
        P(None, "an"),
        P("an", None),
        P(),
        P(),
        P(("sa", "an"), None, None),
        P("sa"),
    )
    return jax.shard_map(
        shards, mesh=mesh, in_specs=placed, out_specs=P("sa", "an"), check_vma=False
    )
```

```python
import functools

import jax
import jax.numpy as jnp
from jax import lax
from jax.experimental import pallas as pl
from jax.experimental.pallas import tpu as pltpu
from jax.sharding import PartitionSpec as P

HEAD = 128
GROUP = 64
NEIGH = 2
EPS = 1e-06
SIDE = 4
PLANE = SIDE * SIDE
LINE = 8
FCHUNK = 512
CORES = 2
PAIR = 2
LOG2E = 1.4426950408889634
F32 = jnp.float32
BF16 = jnp.bfloat16


class Gather:
    def __init__(self, number, buf, send, recv, place, first=None):
        self.number, self.buf, self.send, self.recv = number, buf, send, recv
        self.place = place
        first = first or buf.shape[1] // 2
        self.start = (0, first)
        self.rows = (first, buf.shape[1] - first)

    def cut(self, h):
        return pl.ds(self.start[h], self.rows[h])

    def copy(self, lane, h, k, dy, db, part, to):
        rows, first = self.rows[h], self.start[h]
        if part is not None:
            rows = rows // 2
            first += part * rows
        ref = self.buf.at[self.place.block(lane, dy, db), pl.ds(first, rows)]
        return pltpu.make_async_remote_copy(
            src_ref=ref,
            dst_ref=ref,
            send_sem=self.send.at[self.number],
            recv_sem=self.recv.at[self.number, k],
            device_id=to,
            device_id_type=pl.DeviceIdType.MESH,
        )

    def message(self, name, i=0):
        p = self.place
        up, dn, pair = p.ring(1), p.ring(3), p.pair
        if name == "a_up":
            return 0, 0, (0, 0), (3, 0), None, up
        if name == "a_dn":
            return 0, 1, (0, 0), (1, 0), None, dn
        if name == "a_up2":
            return 0, 2, (3, 0), (2, 0), 0, up
        if name == "a_dn2":
            return 0, 3, (1, 0), (2, 0), 1, dn
        if name == "a_pair":
            return 0, 4 + i, (i, 0), (i, 1), None, pair
        if name == "b_pair":
            return 1, 8, (0, 0), (0, 1), None, pair
        if name == "b_up":
            return 1, 9 + i, (0, i), (3, i), None, up
        if name == "b_dn":
            return 1, 11 + i, (0, i), (1, i), None, dn
        if name == "b_up2":
            return 1, 13 + i, (3, i), (2, i), 0, up
        assert name == "b_dn2"
        return 1, 15 + i, (1, i), (2, i), 1, dn

    def go(self, name, i=0):
        h, k, sent, _, part, to = self.message(name, i)
        self.copy(0, h, k, *sent, part, to).start()

    def get(self, name, i=0):
        h, k, _, got, part, to = self.message(name, i)
        self.copy(0, h, k, *got, part, to).wait_recv()

    def across(self, lane, unit):
        h, dy, db = unit
        k = ROUTED + h * 8 + dy * PAIR + db
        return self.copy(lane, h, k, dy, db, None, self.place.twin)

    def share(self, units):
        for unit in units:
            self.across(0, unit).start()

    def shared(self, event):
        for unit in UNITS[event]:
            self.across(1, unit).wait_recv()

    def own(self, h):
        if h == 0:
            self.go("a_up")
            self.go("a_dn")
            self.go("a_pair", 0)
        else:
            self.go("b_pair")
            self.go("b_up", 0)
            self.go("b_dn", 0)
        self.share([UNITS[0][h]])

    def own_both(self):
        self.go("b_pair")
        self.go("a_up")
        self.go("a_dn")
        self.go("a_pair", 0)
        self.go("b_up", 0)
        self.go("b_dn", 0)
        self.share(UNITS[0])

    def event(self, e):
        if e == 1:
            self.get("a_up")
            self.go("a_up2")
            self.go("a_pair", 3)
            self.get("a_dn")
            self.go("a_dn2")
            self.go("a_pair", 1)
            self.get("b_pair")
            self.go("b_up", 1)
            self.go("b_dn", 1)
        elif e == 2:
            self.get("b_up", 0)
            self.go("b_up2", 0)
            self.get("b_dn", 0)
            self.go("b_dn2", 0)
            self.get("a_pair", 0)
        elif e == 3:
            self.get("a_up2")
            self.get("a_dn2")
            self.go("a_pair", 2)
        elif e == 4:
            self.get("b_up", 1)
            self.go("b_up2", 1)
            self.get("b_dn", 1)
            self.go("b_dn2", 1)
        elif e == 5:
            self.get("a_pair", 3)
            self.get("a_pair", 1)
        elif e in (6, 7):
            self.get("b_up2", e - 6)
            self.get("b_dn2", e - 6)
        else:
            self.get("a_pair", 2)
        self.share(UNITS[e])

    def sent(self):
        ref = self.buf.at[pl.ds(0, PLANE - 1)]
        pltpu.make_async_remote_copy(
            src_ref=ref, dst_ref=ref, send_sem=self.send.at[self.number],
            recv_sem=self.recv.at[self.number, 0], device_id=self.place.pair,
            device_id_type=pl.DeviceIdType.MESH,
        ).wait_send()


ROUTED = 17
SWAP = 33
UNITS = {
    0: [(0, 0, 0), (1, 0, 0)],
    1: [(0, 3, 0), (0, 1, 0), (1, 0, 1)],
    2: [(1, 3, 0), (1, 1, 0), (0, 0, 1)],
    3: [(0, 2, 0)],
    4: [(1, 3, 1), (1, 1, 1)],
    5: [(0, 3, 1), (0, 1, 1)],
    6: [(1, 2, 0)],
    7: [(1, 2, 1)],
    8: [(0, 2, 1)],
}


class Place:
    def __init__(self):
        self.row = lax.axis_index("sa")
        self.me = lax.axis_index("an")
        self.x, self.c = self.row // CORES, self.row % CORES
        self.y, self.z = self.me // SIDE, self.me % SIDE
        self.s, self.b = self.z // PAIR, self.z % PAIR
        self.foreign = (self.c + self.s) % 2
        self.outer = self.y * SIDE + self.outer_z(self.z)
        self.mine = self.block(0, 0, 0)
        self.pair = {"sa": self.row, "an": self.y * SIDE + self.s * PAIR + 1 - self.b}
        self.twin = {"sa": self.row + 1 - 2 * self.c, "an": self.me}
        self.partner = {"sa": self.row + 1 - 2 * self.c, "an": self.outer}
        self.holder = {"sa": self.row, "an": self.outer}

    def outer_z(self, z):
        return (z + 2 * (z % PAIR) + 3) % SIDE

    def ring(self, dy):
        return {"sa": self.row, "an": ((self.y + dy) % SIDE) * SIDE + self.z}

    def block(self, lane, dy, db):
        foreign = (self.foreign + lane) % 2
        b = (self.b + db) % PAIR
        z = self.s * PAIR + b
        return ((self.y + dy) % SIDE) * SIDE + (z + foreign * (2 * b + 3)) % SIDE

    def task_of(self, an):
        y, z = an // SIDE, an % SIDE
        foreign = (self.c + z // PAIR) % 2
        return y * SIDE + (z + foreign * (2 * (z % PAIR) + 3)) % SIDE


def repeat(first, last, step):
    def one(k, carry):
        step(k)
        return carry

    lax.fori_loop(first, last, one, 0)


def either(flag, yes, no):
    pl.when(flag == 1)(yes)
    pl.when(flag == 0)(no)


def visit(own, shared, work):
    for h in (0, 1):
        units = [(0,) + unit[1:] for unit in own if unit[0] == h]
        units += [(1,) + unit[1:] for unit in shared if unit[0] == h]

        def one(i):
            picked = []
            for column in zip(*units):
                value = jnp.int32(column[0])
                for k in range(1, len(column)):
                    value = jnp.where(i == k, jnp.int32(column[k]), value)
                picked.append(value)
            lane, dy, db = picked
            work(lane, h, dy, db)

        if units:
            repeat(0, len(units), one)


def body(
    mine_req, table, states, w_query, w_key, w_value, w_out, enc_up, enc_down, nearby, out,
    sgat, egat, agat, wcol, wq, wkv, wrow, up, down, pool,
    wide, normed, qs, keys, vals, total, arrived, other_table, task_req, slots,
    send, swapped, recv, wsend, wrecv, lsend, lrecv, qsend, qrecv, local, wsem,
):
    p = Place()
    row, me, x, b = p.row, p.me, p.x, p.b
    tokens, width = states.shape
    wrows = w_out.shape[0] // LINE
    chunks = enc_up.shape[1] // FCHUNK
    share = x * PAIR + b

    def remote(src, dst, ssem, rsem, to):
        return pltpu.make_async_remote_copy(
            src_ref=src, dst_ref=dst, send_sem=ssem, recv_sem=rsem,
            device_id=to, device_id_type=pl.DeviceIdType.MESH,
        )

    load_states = pltpu.make_async_copy(states, sgat.at[me], local.at[0])
    stage_states = pltpu.make_async_copy(states, qs, local.at[0])
    load_rows = pltpu.make_async_copy(
        w_out.at[pl.ds(x * PAIR * wrows, PAIR * wrows)], wrow, local.at[1]
    )
    load_pool = pltpu.make_async_copy(nearby, pool, local.at[2])
    load_query = pltpu.make_async_copy(w_query, wq, local.at[3])
    load_key = pltpu.make_async_copy(w_key, wkv.at[:, pl.ds(0, width)], local.at[4])
    load_value = pltpu.make_async_copy(w_value, wkv.at[:, pl.ds(width, width)], local.at[5])
    load_column = pltpu.make_async_copy(
        w_out.at[
            pl.ds(pl.multiple_of(share * wrows, wrows), wrows),
            pl.ds(pl.multiple_of(p.mine * width, width), width),
        ],
        wcol.at[me, share],
        local.at[6],
    )

    def load_up(f):
        cut = pl.ds(pl.multiple_of(f * FCHUNK, FCHUNK), FCHUNK)
        return pltpu.make_async_copy(enc_up.at[:, cut], up.at[:, cut], wsem.at[0, f])

    def load_down(f):
        cut = pl.ds(pl.multiple_of(f * FCHUNK, FCHUNK), FCHUNK)
        return pltpu.make_async_copy(enc_down.at[cut], down.at[cut], wsem.at[1, f])

    def load_weights():
        load_key.start()
        load_value.start()
        load_query.start()

    barrier = pltpu.get_barrier_semaphore()

    def greet(to):
        pl.semaphore_signal(barrier, inc=1, device_id=to, device_id_type=pl.DeviceIdType.MESH)

    def along(dx):
        return {"sa": ((x + dx) % SIDE) * CORES + p.c, "an": me}

    greet(p.partner)
    greet(p.twin)
    repeat(1, PLANE, lambda k: greet({"sa": row, "an": (me + k) % PLANE}))
    greet(along(1))
    greet(along(3))

    load_pool.start()
    load_rows.start()
    repeat(0, chunks // 2, lambda f: (load_up(f).start(), load_down(f).start()))
    either(p.foreign, stage_states.start, load_states.start)
    repeat(chunks // 2, chunks, lambda f: (load_up(f).start(), load_down(f).start()))
    load_column.start()
    pl.when(p.foreign == 0)(load_weights)

    span, own = pool.shape[1], pool.shape[0]
    requests = mine_req.shape[0]
    low, high = jnp.int32(own - 1), jnp.int32(0)
    for k in range(requests):
        offset = mine_req[k] - me * own
        here = (offset >= 0) & (offset < own)
        low = jnp.where(here, jnp.minimum(low, offset), low)
        high = jnp.where(here, jnp.maximum(high, offset), high)
    load_pool.wait()
    for slot, chosen in enumerate((low, high)):
        rows = pool[chosen].astype(F32)
        cut = pl.ds(slot * span, span)
        wide[cut] = rows
        square = jnp.mean(rows * rows, axis=-1, keepdims=True)
        normed[cut] = (rows * lax.rsqrt(square + EPS)).astype(BF16)

    def encode_chunk(f):
        load_up(f).wait()
        load_down(f).wait()
        cut = pl.ds(pl.multiple_of(f * FCHUNK, FCHUNK), FCHUNK)
        pre = jnp.dot(normed[...], up[:, cut], preferred_element_type=F32)
        hidden = (0.5 * pre * (1.0 + lax.erf(pre * 0.5**0.5))).astype(BF16)
        wide[...] += jnp.dot(hidden, down[cut], preferred_element_type=F32)

    early = 3
    repeat(0, early, encode_chunk)
    pl.semaphore_wait(barrier, PLANE - 1 + 4)

    gs = Gather(0, sgat, send, recv, p, first=7 * tokens // 16)
    ge = Gather(1, egat, send, recv, p)
    ga = Gather(2, agat, send, recv, p)

    def swap(gather, h, src, to_slot):
        cut, number = gather.cut(h), gather.number
        return remote(
            src.at[cut], gather.buf.at[to_slot, cut],
            swapped.at[number, h], recv.at[number, SWAP + h], p.partner,
        )

    def plane_copy(k):
        an = (me + k) % PLANE
        part = an % PAIR
        task = p.task_of(an)
        return remote(
            wrow.at[
                pl.ds(pl.multiple_of(part * wrows, wrows), wrows),
                pl.ds(pl.multiple_of(task * width, width), width),
            ],
            wcol.at[me, x * PAIR + part],
            wsend.at[0],
            wrecv.at[0],
            {"sa": row, "an": an},
        )

    def home_states():
        load_states.wait()
        gs.own_both()

    def swap_states():
        stage_states.wait()
        for h in (0, 1):
            swap(gs, h, qs, me).start()

    either(p.foreign, swap_states, home_states)
    load_rows.wait()
    repeat(1, PLANE, lambda k: plane_copy(k).start())
    table_copy = remote(table, other_table, qsend.at[0], qrecv.at[0], p.twin)
    table_copy.start()
    repeat(early, chunks, encode_chunk)

    def plane_all():
        ref = wcol.at[pl.ds(0, PLANE - 1), share]
        return remote(ref, ref, wsend.at[0], wrecv.at[0], p.pair)

    def across(held):
        ref = wcol.at[:, held]
        return remote(ref, ref, lsend.at[0], lrecv.at[0], p.holder)

    def along_copy(k, held, to, part=None):
        blocks = pl.ds(0, PLANE) if part is None else pl.ds(part * (PLANE // 2), PLANE // 2)
        ref = wcol.at[blocks, pl.ds((held % SIDE) * PAIR, PAIR)]
        return remote(ref, ref, lsend.at[k], lrecv.at[k], along(to))

    def spread1():
        load_column.wait()
        plane_all().wait_recv()
        across(share).start()

    def spread2():
        across(share + 1 - 2 * b).wait_recv()
        along_copy(1, x, 1).start()
        along_copy(2, x, 3).start()

    def spread3():
        along_copy(1, x + 3, 1).wait_recv()
        along_copy(3, x + 3, 1, 0).start()
        along_copy(2, x + 1, 3).wait_recv()
        along_copy(4, x + 1, 3, 1).start()

    def spread4():
        along_copy(3, x + 2, 1, 0).wait_recv()
        along_copy(4, x + 2, 3, 1).wait_recv()

    def spread_sent():
        across(share).wait_send()
        along_copy(1, x, 1).wait_send()
        along_copy(2, x, 3).wait_send()
        along_copy(3, x, 1, 0).wait_send()
        along_copy(4, x, 3, 1).wait_send()

    def swap_encoded():
        normed[...] = wide[...].astype(BF16)
        for h in (0, 1):
            swap(ge, h, normed, me).start()
        for h in (0, 1):
            swap(gs, h, qs, p.outer).wait_recv()
            gs.own(h)

    def keep_encoded():
        egat[me] = wide[...].astype(BF16)
        ge.own_both()

    either(p.foreign, swap_encoded, keep_encoded)

    weight_copies = (
        remote(wkv, wkv, qsend.at[1], qrecv.at[1], p.holder),
        remote(wq, wq, qsend.at[2], qrecv.at[2], p.holder),
    )

    def give_weights():
        load_key.wait()
        load_value.wait()
        load_query.wait()
        for copy in weight_copies:
            copy.start()

    def late_encoded():
        for h in (0, 1):
            swap(ge, h, normed, p.outer).wait_recv()
            ge.own(h)
        spread1()

    pl.when(p.foreign == 1)(late_encoded)
    gs.event(1)
    table_copy.wait_recv()
    task_copies = [
        pltpu.make_async_copy(src, task_req, local.at[7]) for src in (other_table, table)
    ]
    either(p.foreign, task_copies[0].start, task_copies[1].start)

    def find_slot(k):
        wanted = task_req[0, k]
        owner = wanted // own
        later = jnp.int32(0)
        for j in range(requests):
            other = task_req[0, j]
            later = jnp.where((other < wanted) & (other >= owner * own), jnp.int32(1), later)
        slots[k] = owner * NEIGH + later

    def project(lane, h, dy, db):
        block = p.block(lane, dy, db)
        slot = block * NEIGH + h
        cut = pl.ds(pl.multiple_of(h * span, span), span)
        both = jnp.dot(egat[block, cut], wkv[...], preferred_element_type=F32)
        keys[slot] = both[:, :width].astype(BF16)
        vals[slot] = both[:, width:].astype(BF16)

    query_early = [u for e in range(5) for u in UNITS[e]]
    query_late = [u for e in range(5, 9) for u in UNITS[e]]

    def query_part(units, last):
        for h in (0, 1):
            blocks = [(lane, dy, db) for lane in (0, 1) for (k, dy, db) in units if k == h]
            rows = gs.rows[h] // 2

            def tile(t):
                cut = pl.ds(pl.multiple_of(gs.start[h] + t * rows, 32), rows)
                acc = total[cut] if last else jnp.zeros((rows, width), F32)
                for at in blocks:
                    j = p.block(*at)
                    acc = acc + jnp.dot(
                        sgat[j, cut], wq[pl.ds(pl.multiple_of(j * width, width), width)],
                        preferred_element_type=F32,
                    )
                if last:
                    qs[cut] = acc.astype(BF16)
                else:
                    total[cut] = acc

            repeat(0, 2, tile)

    gs.event(2)
    def spread1_then_weights():
        spread1()
        give_weights()

    either(p.foreign, spread2, spread1_then_weights)
    ge.event(1)
    gs.event(3)
    pl.when(p.foreign == 0)(spread2)
    ge.event(2)
    either(p.foreign, task_copies[0].wait, task_copies[1].wait)
    repeat(0, requests, find_slot)
    pl.when(p.foreign == 1)(weight_copies[0].wait_recv)
    visit(UNITS[0] + UNITS[1], [], project)
    ge.event(3)
    spread3()
    visit(UNITS[2] + UNITS[3], [], project)
    gs.event(4)
    for event in (0, 1):
        ge.shared(event)
    visit([], UNITS[0] + UNITS[1], project)
    ge.event(4)
    for event in (2, 3):
        ge.shared(event)
    visit(UNITS[4], UNITS[2] + UNITS[3], project)
    for event in range(5):
        gs.shared(event)

    def sent_states():
        for h in (0, 1):
            swap(gs, h, qs, me).wait_send()

    def foreign_ready():
        weight_copies[1].wait_recv()
        sent_states()

    gs.event(5)
    ge.shared(4)
    visit([], UNITS[4], project)
    pl.when(p.foreign == 1)(foreign_ready)
    query_part(query_early, False)
    for event in (6, 7, 8):
        gs.event(event)
    ge.event(5)
    visit(UNITS[5], [], project)
    for event in (5, 6, 7, 8):
        gs.shared(event)
    for event in (6, 7, 8):
        ge.event(event)
    query_part(query_late, True)
    ge.shared(5)
    ge.shared(6)
    visit(UNITS[6] + UNITS[7] + UNITS[8], UNITS[5] + UNITS[6], project)
    ge.shared(7)
    ge.shared(8)
    visit([], UNITS[7] + UNITS[8], project)

    power = float(HEAD) ** -0.5 * LOG2E

    def attend(t):
        scores, held = [], []
        for g in (2 * t, 2 * t + 1):
            one, two = slots[NEIGH * g], slots[NEIGH * g + 1]
            q = qs[pl.ds(pl.multiple_of(g * GROUP, GROUP), GROUP)]
            k = jnp.concatenate([keys[one], keys[two]], axis=0)
            held.append(jnp.concatenate([vals[one], vals[two]], axis=0))
            for h in range(width // HEAD):
                part = slice(h * HEAD, (h + 1) * HEAD)
                scores.append(lax.dot_general(
                    q[:, part], k[:, part], (((1,), (1,)), ((), ())),
                    preferred_element_type=F32,
                ))
        weights = [jnp.exp2((v - jnp.max(v, axis=-1, keepdims=True)) * power) for v in scores]
        probs = [
            (w * (1.0 / jnp.sum(w, axis=-1, keepdims=True))).astype(BF16) for w in weights
        ]
        heads = width // HEAD
        rows = []
        for i in range(2):
            done = [
                jnp.dot(
                    probs[i * heads + h], held[i][:, h * HEAD : (h + 1) * HEAD],
                    preferred_element_type=F32,
                )
                for h in range(heads)
            ]
            rows.append(jnp.concatenate(done, axis=1))
        cut = pl.ds(pl.multiple_of(2 * t * GROUP, 2 * GROUP), 2 * GROUP)
        agat[p.mine, cut] = jnp.concatenate(rows, axis=0).astype(BF16)

    pairs = tokens // GROUP // 2
    repeat(0, pairs // 2, attend)
    ga.own(0)
    repeat(pairs // 2, pairs, attend)
    ga.own(1)

    total[...] = jnp.zeros_like(total)

    def add_output(lane, h, dy, db):
        j = p.block(lane, dy, db)
        cut = pl.ds(pl.multiple_of(h * half, half), half)
        total[cut] += jnp.dot(
            agat[j, cut], wcol[j].reshape(width, width), preferred_element_type=F32
        )

    half = tokens // 2

    def swap_out(h):
        cut = pl.ds(h * half, half)
        return remote(
            qs.at[cut], arrived.at[cut], swapped.at[2, h], recv.at[2, SWAP + h], p.partner
        )

    def finish(h):
        cut = pl.ds(h * half, half)

        def give():
            qs[cut] = total[cut].astype(BF16)
            swap_out(h).start()

        def keep():
            out[cut] = total[cut].astype(BF16)

        either(p.foreign, give, keep)

    ga.event(1)
    ga.event(2)
    spread4()
    ga.shared(0)
    visit(UNITS[0] + UNITS[1], UNITS[0], add_output)
    for event in (3, 4):
        ga.event(event)
        ga.shared(event - 2)
        visit(UNITS[event - 1], UNITS[event - 2], add_output)
    ga.shared(3)
    visit(UNITS[4], UNITS[3], add_output)
    ga.event(5)
    ga.event(6)
    ga.shared(4)
    visit(UNITS[5] + UNITS[6], UNITS[4], add_output)
    ga.event(7)
    ga.shared(5)
    ga.shared(6)
    visit(UNITS[7], UNITS[5] + UNITS[6], add_output)
    ga.shared(7)
    visit([], UNITS[7], add_output)
    finish(1)
    ga.event(8)
    visit(UNITS[8], [], add_output)
    ga.shared(8)
    visit([], UNITS[8], add_output)
    finish(0)

    def take():
        for h in (1, 0):
            cut = pl.ds(h * half, half)
            swap_out(h).wait_recv()
            out[cut] = arrived[cut]

    pl.when(p.foreign == 1)(take)

    for gather in (gs, ge, ga):
        gather.sent()
    table_copy.wait_send()

    def sent_foreign():
        for h in (0, 1):
            swap(ge, h, normed, me).wait_send()
            swap_out(h).wait_send()

    def sent_home():
        for copy in weight_copies:
            copy.wait_send()

    either(p.foreign, sent_foreign, sent_home)
    plane_all().wait_send()
    spread_sent()


def shards(
    decoder_states, w_query, w_key, w_value, w_out, enc_up, enc_down, neighbour_inputs, requests
):
    tokens, width = decoder_states.shape
    _, span, features = neighbour_inputs.shape
    hbm = pl.BlockSpec(memory_space=pl.ANY)
    slots = PLANE * NEIGH
    chunks = enc_up.shape[1] // FCHUNK
    return pl.pallas_call(
        body,
        out_shape=pltpu.VMEM((tokens, width), BF16),
        in_specs=[
            pl.BlockSpec(memory_space=pltpu.SMEM), pl.BlockSpec(memory_space=pltpu.VMEM)
        ] + [hbm] * 8,
        out_specs=pl.BlockSpec(memory_space=pltpu.VMEM),
        scratch_shapes=[
            pltpu.VMEM((PLANE, tokens, width), BF16),
            pltpu.VMEM((PLANE, NEIGH * span, features), BF16),
            pltpu.VMEM((PLANE, tokens, width), BF16),
            pltpu.VMEM((PLANE, LINE, w_out.shape[0] // LINE, width), BF16),
            pltpu.VMEM(w_query.shape, BF16),
            pltpu.VMEM((features, 2 * width), BF16),
            pltpu.VMEM((PAIR * w_out.shape[0] // LINE, w_out.shape[1]), BF16),
            pltpu.VMEM(enc_up.shape, BF16),
            pltpu.VMEM(enc_down.shape, BF16),
            pltpu.VMEM(neighbour_inputs.shape, BF16),
            pltpu.VMEM((NEIGH * span, features), F32),
            pltpu.VMEM((NEIGH * span, features), BF16),
            pltpu.VMEM((tokens, width), BF16),
            pltpu.VMEM((slots, span, width), BF16),
            pltpu.VMEM((slots, span, width), BF16),
            pltpu.VMEM((tokens, width), F32),
            pltpu.VMEM((tokens, width), BF16),
            pltpu.VMEM((1, requests.shape[0]), jnp.int32),
            pltpu.SMEM((1, requests.shape[0]), jnp.int32),
            pltpu.SMEM(requests.shape, jnp.int32),
            pltpu.SemaphoreType.DMA((3,)),
            pltpu.SemaphoreType.DMA((3, 2)),
            pltpu.SemaphoreType.DMA((3, SWAP + 2)),
            pltpu.SemaphoreType.DMA((1,)),
            pltpu.SemaphoreType.DMA((1,)),
            pltpu.SemaphoreType.DMA((5,)),
            pltpu.SemaphoreType.DMA((5,)),
            pltpu.SemaphoreType.DMA((3,)),
            pltpu.SemaphoreType.DMA((3,)),
            pltpu.SemaphoreType.DMA((8,)),
            pltpu.SemaphoreType.DMA((2, chunks)),
        ],
        compiler_params=pltpu.CompilerParams(
            collective_id=0, has_side_effects=True, vmem_limit_bytes=62 * 2**20
        ),
    )(
        requests, requests[None, :], decoder_states, w_query, w_key, w_value, w_out,
        enc_up, enc_down, neighbour_inputs,
    )


def solution(mesh):
    placed = (
        P("sa", "an"),
        P(None, "an"),
        P(None, "an"),
        P(None, "an"),
        P("an", None),
        P(),
        P(),
        P(("sa", "an"), None, None),
        P("sa"),
    )
    return jax.shard_map(
        shards, mesh=mesh, in_specs=placed, out_specs=P("sa", "an"), check_vma=False
    )
```
